256 devices in a mesh: depth: 64 (over y, z, core), lat: 4 (over x).
Axes of the slice: x: 4, y: 4, z: 8, core: 2. Of those that a mesh axis runs over, the one named last changes fastest.
Arguments:
- sources: float32 [64, 2, 64, 4096], P('depth', None, None, 'lat'), may hold values from -6 to 6
- down_expand: float32 [64, 2, 64, 4096], P('depth', None, None, 'lat'), may hold values from -0.75 to 0.75
- down_project: float32 [64, 2, 64, 4096], P('depth', None, None, 'lat'), may hold values from -0.09375 to 0.09375
- up_expand: float32 [64, 2, 64, 4096], P('depth', None, None, 'lat'), may hold values from -0.75 to 0.75
- up_project: float32 [64, 2, 64, 4096], P('depth', None, None, 'lat'), may hold values from -0.09375 to 0.09375
- down_decay: float32 [64, 64], P('depth'), may hold values from 0.3 to 0.8
- up_decay: float32 [64, 64], P('depth'), may hold values from 0.3 to 0.8
- active_list: int32 [64, 64], P('depth'), may hold values from 0 to 63, each once within a row
- active_count: int32 [64], P('depth'), may hold values from 1 to 64
- incident_down: float32 [2, 64, 4096], P(None, None, 'lat'), may hold values from -6 to 6
- incident_up: float32 [2, 64, 4096], P(None, None, 'lat'), may hold values from -6 to 6
Outputs:
- field: float32 [64, 2, 64, 4096], P('depth', None, None, 'lat')
The draws below stay inside these ranges and needn't reach their ends.
Inputs may be any that keep to these rules, and one draw needn't show every extreme that they name: Each row of active_list holds every source number once.
All inputs are finite; a program needn't handle non-finite values.
Results may differ from the reference program's by a relative error of at most 0.0003.
Values sent between devices are 32-bit elements; how exact they have to be, the bound alone decides.
A program may use at most 64 MiB of HBM per device.

```python
import math
import jax
import jax.numpy as jnp
from jax import lax

SRC = 64
RANK = 64
LAT = 4096
GROUPS = 64


def plant(entries, rng, low, largest):
    longest = entries.shape.index(max(entries.shape))
    spots = []
    for shift in (0, 1):
        where = [jax.random.randint(jax.random.fold_in(rng, axis), (), 0, length) for axis, length in enumerate(entries.shape)]
        where[longest] = (where[longest] + shift) % entries.shape[longest]
        spots.append(tuple(where))
    return entries.at[spots[0]].set(low).at[spots[1]].set(largest)


def shard_levels(key, shape, cuts, low, top_value):
    loudness, own = 1.0, jax.random.fold_in(key, 6)
    for axis_at, parts in cuts:
        heights = jnp.exp(jax.random.uniform(jax.random.fold_in(own, axis_at), (parts,), jnp.float32, low / len(cuts), top_value / len(cuts)))
        loudness = loudness * jnp.repeat(heights, shape[axis_at] // parts).reshape([-1 if axis == axis_at else 1 for axis in range(len(shape))])
    return loudness


def gaussian(own_key, shape, deviation, limit, shards=(), held_as=jnp.bfloat16):
    gain = shard_levels(own_key, shape, shards, -0.22, 0.18) if shards else 1.0
    array = jax.random.normal(own_key, shape, jnp.float32) * deviation * gain
    return jnp.minimum(jnp.maximum(array, -limit), limit).astype(held_as)


def setup_inputs(seed: int = 0) -> dict:
    key_list = jax.random.split(jax.random.key(seed), 12)
    return {
        "sources": gaussian(key_list[0], (GROUPS, 2, SRC, LAT), 1.0, 6.0, ((0, 64), (3, 4)), jnp.float32),
        "down_expand": gaussian(key_list[1], (GROUPS, 2, RANK, LAT), RANK ** -0.5, 0.75, ((0, 64), (3, 4)), jnp.float32),
        "down_project": gaussian(key_list[2], (GROUPS, 2, RANK, LAT), LAT ** -0.5, 0.09375, ((0, 64), (3, 4)), jnp.float32),
        "up_expand": gaussian(key_list[3], (GROUPS, 2, RANK, LAT), RANK ** -0.5, 0.75, ((0, 64), (3, 4)), jnp.float32),
        "up_project": gaussian(key_list[4], (GROUPS, 2, RANK, LAT), LAT ** -0.5, 0.09375, ((0, 64), (3, 4)), jnp.float32),
        "down_decay": jnp.clip(jnp.exp(math.log(0.8) - 0.98082923 * jax.random.uniform(key_list[5], (GROUPS, RANK), jnp.float32) ** shard_levels(key_list[5], (GROUPS, RANK), ((0, 64),), -0.2, 0.2)), 0.3, 0.8),
        "up_decay": jnp.clip(jnp.exp(math.log(0.8) - 0.98082923 * jax.random.uniform(key_list[6], (GROUPS, RANK), jnp.float32) ** shard_levels(key_list[6], (GROUPS, RANK), ((0, 64),), -0.2, 0.2)), 0.3, 0.8),
        "active_list": jax.vmap(lambda own: jax.random.permutation(own, SRC))(jax.random.split(key_list[7], GROUPS)).reshape((GROUPS, SRC)).astype(jnp.int32),
        "active_count": plant(jax.random.randint(key_list[8], (GROUPS,), 1, SRC + 1), jax.random.fold_in(key_list[8], 1), 1, SRC).astype(jnp.int32),
        "incident_down": gaussian(key_list[9], (2, SRC, LAT), 1.0, 6.0, ((2, 4),), jnp.float32),
        "incident_up": gaussian(key_list[10], (2, SRC, LAT), 1.0, 6.0, ((2, 4),), jnp.float32),
    }


def contract(left, right):
    hp = lax.Precision.HIGHEST
    dims = (((1,), (1,)), ((), ()))
    def prod(a, b):
        return lax.dot_general(a, b, dims, precision=hp, preferred_element_type=jnp.float32)
    real = prod(left[0], right[0]) - prod(left[1], right[1])
    imag = prod(left[0], right[1]) + prod(left[1], right[0])
    return jnp.stack([real, imag])


def expand(coef, basis):
    hp = lax.Precision.HIGHEST
    dims = (((0,), (0,)), ((), ()))
    def prod(a, b):
        return lax.dot_general(a, b, dims, precision=hp, preferred_element_type=jnp.float32)
    real = prod(coef[0], basis[0]) - prod(coef[1], basis[1])
    imag = prod(coef[0], basis[1]) + prod(coef[1], basis[0])
    return jnp.stack([real, imag])


def reference(sources, down_expand, down_project, up_expand, up_project, down_decay, up_decay, active_list, active_count, incident_down, incident_up):
    places = jnp.arange(SRC, dtype=jnp.int32)
    valid = (places[None, :] < active_count[:, None]).astype(jnp.float32)
    hits = (active_list[:, :, None] == places[None, None, :]).astype(jnp.float32)
    mask = jnp.sum(valid[:, :, None] * hits, axis=1)
    local = sources * mask[:, None, :, None]

    def sweep(prev, items):
        wave, proj, basis, decay = items
        coef = decay[None, :, None] * contract(proj, prev)
        term = expand(coef, basis)
        return wave + term, term

    _, down_terms = lax.scan(sweep, incident_down, (local, down_project, down_expand, down_decay))
    _, up_terms = lax.scan(sweep, incident_up, (local, up_project, up_expand, up_decay), reverse=True)
    return local + down_terms + up_terms
```

```python
import functools

import jax
import jax.numpy as jnp
from jax import lax
from jax.experimental import pallas as pl
from jax.experimental.pallas import tpu as pltpu
from jax.sharding import PartitionSpec as P

F32 = jnp.float32
BF16 = jnp.bfloat16
MESH = pl.DeviceIdType.MESH
CHUNKS = 4


def halves(value):
    high = value.astype(BF16)
    return high, (value - high.astype(F32)).astype(BF16)


def dot(left, right):
    return lax.dot_general(left, right, (((1,), (0,)), ((), ())), preferred_element_type=F32)


def dot_rows(left, right):
    return lax.dot_general(left, right, (((1,), (1,)), ((), ())), preferred_element_type=F32)


def lanes_of(shape):
    return lax.broadcasted_iota(jnp.int32, shape, 1)


def compose(later, earlier):
    n = later.shape[0] // 2
    real, imag = later[:n], later[n:]
    left = lanes_of(real.shape) < n
    top = jnp.where(left, real, -pltpu.roll(imag, n, 1))
    low = jnp.where(left, imag, pltpu.roll(real, n, 1))
    lhs_h, lhs_l = halves(jnp.concatenate([top, low], axis=0))
    rhs_h, rhs_l = halves(earlier)
    out = dot(jnp.concatenate([lhs_h, lhs_l], axis=1), jnp.concatenate([rhs_h, rhs_h], axis=0))
    out = out + dot(lhs_h, rhs_l)
    return out + jnp.where(lanes_of(later.shape) < n, 0.0, later)


def kernel(
    dims,
    src_hbm, dexp_hbm, dproj_hbm, uexp_hbm, uproj_hbm, ddec_ref, udec_ref, list_ref, count_ref, incd_hbm, incu_hbm,
    out_ref,
    src, exps, inc, proj, wh, wl, xsend, xrecv, state, zsend, zrecv, ysend, yrecv, start, qown, qsend, qrecv, tother,
    load_sem, psend_sem, precv_sem, xsend_sem, xrecv_sem, tsend_sem, trecv_sem, zsend_sem, zrecv_sem,
    ysend_sem, yrecv_sem, qsend_sem, qrecv_sem,
):
    ny, nz, nx = dims
    groups = ny * nz * 2
    rounds = nz.bit_length() - 1
    masks = [1 << k for k in range(rounds - 1)] + [nz - 1]
    g = lax.axis_index("depth")
    x = lax.axis_index("lat")
    core = lax.rem(g, 2)
    z = lax.rem(lax.div(g, 2), nz)
    y = lax.div(g, 2 * nz)
    zz = jnp.where(core == 0, z, nz - 1 - z)
    yy = jnp.where(core == 0, y, ny - 1 - y)
    mate = g + 1 - 2 * core
    is_first = g == 0
    is_last = g == groups - 1
    begins = jnp.logical_and(yy == 0, zz == 0)

    def place(to_y, to_z):
        return (to_y * nz + to_z) * 2 + core

    def xor(value, mask):
        out = value
        for bit in range(rounds):
            if mask >> bit & 1:
                set_ = lax.rem(lax.div(value, 1 << bit), 2)
                out = out + (1 << bit) * (1 - 2 * set_)
        return out

    z_peers = [place(y, xor(z, mask)) for mask in masks]
    y_peers = [place(lax.rem(y + o, ny), z) for o in range(1, ny)]

    barrier = pltpu.get_barrier_semaphore()
    for o in range(1, nx):
        pl.semaphore_signal(barrier, inc=1, device_id=(g, lax.rem(x + o, nx)), device_id_type=MESH)
    for peer in z_peers + y_peers:
        pl.semaphore_signal(barrier, inc=1, device_id=(peer, x), device_id_type=MESH)

    @pl.when(jnp.logical_not(is_first))
    def _():
        pl.semaphore_signal(barrier, inc=1, device_id=(g - 1, x), device_id_type=MESH)

    @pl.when(jnp.logical_not(is_last))
    def _():
        pl.semaphore_signal(barrier, inc=1, device_id=(g + 1, x), device_id_type=MESH)

    loads = [
        pltpu.make_async_copy(dexp_hbm, exps.at[0], load_sem.at[0]),
        pltpu.make_async_copy(src_hbm, src, load_sem.at[1]),
        pltpu.make_async_copy(uexp_hbm, exps.at[1], load_sem.at[2]),
    ]
    for copy in loads:
        copy.start()

    inc_copies = [
        pltpu.make_async_copy(incd_hbm, inc, load_sem.at[3]),
        pltpu.make_async_copy(incu_hbm, inc, load_sem.at[3]),
    ]
    pl.when(is_first)(inc_copies[0].start)
    pl.when(is_last)(inc_copies[1].start)

    edge = jnp.where(jnp.logical_or(is_first, is_last), 1, 0)
    pl.semaphore_wait(barrier, nx - 1 + len(z_peers) + len(y_peers) + 2 - edge)

    size = proj.shape[3]
    sends = []
    for k in range(CHUNKS):
        rows = pl.ds(k * size, size)
        down = pltpu.make_async_remote_copy(
            src_ref=dproj_hbm.at[:, rows], dst_ref=proj.at[0, k],
            send_sem=psend_sem.at[0, k], recv_sem=precv_sem.at[0, k],
            device_id=(jnp.maximum(g - 1, 0), x), device_id_type=MESH,
        )
        up = pltpu.make_async_remote_copy(
            src_ref=uproj_hbm.at[:, rows], dst_ref=proj.at[1, k],
            send_sem=psend_sem.at[1, k], recv_sem=precv_sem.at[1, k],
            device_id=(jnp.minimum(g + 1, groups - 1), x), device_id_type=MESH,
        )
        own_down = pltpu.make_async_copy(dproj_hbm.at[:, rows], proj.at[1, k], precv_sem.at[1, k])
        own_up = pltpu.make_async_copy(uproj_hbm.at[:, rows], proj.at[0, k], precv_sem.at[0, k])

        @pl.when(jnp.logical_not(is_first))
        def _():
            down.start()

        @pl.when(is_first)
        def _():
            own_down.start()

        @pl.when(jnp.logical_not(is_last))
        def _():
            up.start()

        @pl.when(is_last)
        def _():
            own_up.start()

        sends.append((down, up))

    n = src.shape[1]
    square = (n, n)
    row_at = lax.broadcasted_iota(jnp.int32, square, 0)
    lane_at = lanes_of(square)
    valid = jnp.logical_and(list_ref[...] == row_at, lane_at < count_ref[0])
    mask = jnp.sum(jnp.where(valid, 1.0, 0.0), axis=1, keepdims=True)
    for slot, (dec_ref, load) in enumerate(((ddec_ref, loads[0]), (udec_ref, loads[2]))):
        decay = jnp.sum(jnp.where(row_at == lane_at, dec_ref[...], 0.0), axis=1, keepdims=True)
        load.wait()
        for part in range(2):
            high, low = halves(exps[slot, part] * decay)
            wh[slot, pl.ds(2 * part * n, n)] = high
            wl[slot, pl.ds(2 * part * n, n)] = low
    loads[1].wait()
    for part in range(2):
        high, low = halves(src[part] * mask)
        for slot in range(2):
            wh[slot, pl.ds((2 * part + 1) * n, n)] = high
            wl[slot, pl.ds((2 * part + 1) * n, n)] = low
    for slot, at_edge in ((1, is_first), (0, is_last)):

        @pl.when(at_edge)
        def _():
            inc_copies[0].wait()
            for part in range(2):
                high, low = halves(inc[part])
                wh[slot, pl.ds((2 * part + 1) * n, n)] = high
                wl[slot, pl.ds((2 * part + 1) * n, n)] = low

    x_copies = {}
    for k in range(CHUNKS):
        for slot in range(2):
            sends[k][slot].wait_recv()
            p_h, p_l = halves(proj[slot, k].reshape(2 * size, proj.shape[4]))
            both = dot_rows(jnp.concatenate([p_h, p_l], axis=0), wh[slot])
            total = both[: 2 * size] + both[2 * size :] + dot_rows(p_h, wl[slot])
            first, second = total[:size], total[size:]
            xsend[slot, k, 0] = first[:, : 2 * n] - second[:, 2 * n :]
            xsend[slot, k, 1] = first[:, 2 * n :] + second[:, : 2 * n]
            for o in range(1, nx):
                copy = pltpu.make_async_remote_copy(
                    src_ref=xsend.at[slot, k], dst_ref=xrecv.at[slot, k, o - 1],
                    send_sem=xsend_sem.at[slot, k, o - 1], recv_sem=xrecv_sem.at[slot, k, o - 1],
                    device_id=(g, lax.rem(x + o, nx)), device_id_type=MESH,
                )
                copy.start()
                x_copies[slot, k, o] = copy
    for k in range(CHUNKS):
        for slot in range(2):
            total = xsend[slot, k]
            for o in range(1, nx):
                x_copies[slot, k, o].wait_recv()
                total = total + xrecv[slot, k, o - 1]
            for part in range(2):
                state[slot, pl.ds(part * n + k * size, size)] = total[part]

    swap = pltpu.make_async_remote_copy(
        src_ref=state.at[1 - core], dst_ref=tother, send_sem=tsend_sem, recv_sem=trecv_sem,
        device_id=(mate, x), device_id_type=MESH,
    )
    swap.start()
    wide = state.shape[1:]
    in_map = lanes_of(wide) < n
    mine = state[core]
    initial = jnp.where(in_map, 0.0, state[1 - core])
    qown[...] = mine

    @pl.when(begins)
    def _():
        qown[...] = compose(mine, initial)

    swap.wait_recv()
    total = compose(tother[...], qown[...])
    row = lax.broadcasted_iota(jnp.int32, wide, 0)
    prefix = jnp.where(jnp.logical_and(row == lanes_of(wide), in_map), 1.0, 0.0)
    z_copies = []
    for k in range(rounds):
        zsend[k] = total
        copy = pltpu.make_async_remote_copy(
            src_ref=zsend.at[k], dst_ref=zrecv.at[k], send_sem=zsend_sem.at[k], recv_sem=zrecv_sem.at[k],
            device_id=(z_peers[k], x), device_id_type=MESH,
        )
        copy.start()
        z_copies.append(copy)
        copy.wait_recv()
        theirs = zrecv[k]
        after = lax.rem(lax.div(zz, 1 << k), 2) == 1
        if k == 0:
            joined = theirs
        else:
            joined = compose(prefix, theirs)
        prefix = jnp.where(after, joined, prefix)
        total = compose(jnp.where(after, total, theirs), jnp.where(after, theirs, total))

    ysend[...] = total
    y_copies = []
    for o in range(1, ny):
        to_y = jnp.where(core == 0, lax.rem(y + o, ny), lax.rem(y + ny - o, ny))
        copy = pltpu.make_async_remote_copy(
            src_ref=ysend, dst_ref=yrecv.at[o - 1], send_sem=ysend_sem.at[o - 1], recv_sem=yrecv_sem.at[o - 1],
            device_id=(place(to_y, z), x), device_id_type=MESH,
        )
        y_copies.append(copy)
        pl.when(yy + o < ny)(copy.start)

    @pl.when(yy == 0)
    def _():
        qown[...] = jnp.where(begins, initial, prefix)

    for at in range(1, ny):

        @pl.when(yy == at)
        def _():
            for o in range(at, 0, -1):
                y_copies[o - 1].wait_recv()
            here = yrecv[at - 1]
            for o in range(at - 1, 0, -1):
                here = compose(yrecv[o - 1], here)
            qown[...] = compose(prefix, here)

    qsend[...] = compose(mine, qown[...])
    give = pltpu.make_async_remote_copy(
        src_ref=qsend, dst_ref=qrecv, send_sem=qsend_sem, recv_sem=qrecv_sem,
        device_id=(mate, x), device_id_type=MESH,
    )
    give.start()
    give.wait_recv()

    own, other = qown[...], qrecv[...]
    left = lanes_of((n, 2 * n)) < n
    coefs = []
    for value in (jnp.where(core == 0, own, other), jnp.where(core == 0, other, own)):
        turned = jnp.transpose(value)[n:]
        coefs.append(jnp.concatenate([jnp.where(left, turned, -turned), pltpu.roll(turned, n, 1)], axis=0))
    c_h, c_l = halves(jnp.concatenate(coefs, axis=1))
    c_all = jnp.concatenate([c_h, c_l], axis=0)
    width = src.shape[2]
    step = min(256, width)
    for at in range(0, width, step):
        cols = pl.ds(at, step)
        picks = [(slot, pl.ds(2 * part * n, n)) for slot in range(2) for part in range(2)]
        e_h = jnp.concatenate([wh[slot, rows, cols] for slot, rows in picks], axis=0)
        e_l = jnp.concatenate([wl[slot, rows, cols] for slot, rows in picks], axis=0)
        both = dot(c_all, e_h)
        terms = both[: 2 * n] + both[2 * n :] + dot(c_h, e_l)
        for part in range(2):
            out_ref[part, :, cols] = src[part, :, cols] * mask + terms[part * n : (part + 1) * n]

    for k, (down, up) in enumerate(sends):
        pl.when(jnp.logical_not(is_first))(down.wait_send)
        pl.when(jnp.logical_not(is_last))(up.wait_send)
    for copy in x_copies.values():
        copy.wait_send()
    swap.wait_send()
    for copy in z_copies:
        copy.wait_send()
    for o, copy in enumerate(y_copies, 1):
        pl.when(yy + o < ny)(copy.wait_send)
    give.wait_send()


def sweeps(dims, *args):
    sources, dexp, dproj, uexp, uproj, ddec, udec, active, count, incd, incu = args
    ny, nz, nx = dims
    _, _, n, width = sources.shape
    size = n // CHUNKS
    rounds = nz.bit_length() - 1
    full = (2 * n, 2 * n)
    anywhere = pl.BlockSpec(memory_space=pl.ANY)
    vmem = pl.BlockSpec(memory_space=pltpu.VMEM)
    dma = pltpu.SemaphoreType.DMA
    field = pl.pallas_call(
        functools.partial(kernel, dims),
        out_shape=jax.ShapeDtypeStruct((2, n, width), F32),
        in_specs=[anywhere] * 5 + [vmem] * 3 + [pl.BlockSpec(memory_space=pltpu.SMEM)] + [anywhere] * 2,
        out_specs=vmem,
        scratch_shapes=[
            pltpu.VMEM((2, n, width), F32),
            pltpu.VMEM((2, 2, n, width), F32),
            pltpu.VMEM((2, n, width), F32),
            pltpu.VMEM((2, CHUNKS, 2, size, width), F32),
            pltpu.VMEM((2, 4 * n, width), BF16),
            pltpu.VMEM((2, 4 * n, width), BF16),
            pltpu.VMEM((2, CHUNKS, 2, size, 2 * n), F32),
            pltpu.VMEM((2, CHUNKS, nx - 1, 2, size, 2 * n), F32),
            pltpu.VMEM((2, *full), F32),
            pltpu.VMEM((rounds, *full), F32),
            pltpu.VMEM((rounds, *full), F32),
            pltpu.VMEM(full, F32),
            pltpu.VMEM((ny - 1, *full), F32),
            pltpu.VMEM(full, F32),
            pltpu.VMEM(full, F32),
            pltpu.VMEM(full, F32),
            pltpu.VMEM(full, F32),
            pltpu.VMEM(full, F32),
            dma((4,)),
            dma((2, CHUNKS)),
            dma((2, CHUNKS)),
            dma((2, CHUNKS, nx - 1)),
            dma((2, CHUNKS, nx - 1)),
            dma(()),
            dma(()),
            dma((rounds,)),
            dma((rounds,)),
            dma((ny - 1,)),
            dma((ny - 1,)),
            dma(()),
            dma(()),
        ],
        compiler_params=pltpu.CompilerParams(collective_id=0, has_side_effects=True),
        name="sweeps",
    )(sources[0], dexp[0], dproj[0], uexp[0], uproj[0], ddec, udec, active, count, incd, incu)
    return field[None]


def solution(mesh, ny=4):
    depth, nx = mesh.shape["depth"], mesh.shape["lat"]
    dims = (ny, depth // (2 * ny), nx)
    by_group = P("depth", None, None, "lat")
    return jax.shard_map(
        functools.partial(sweeps, dims),
        mesh=mesh,
        in_specs=(by_group,) * 5
        + (P("depth", None),) * 3
        + (P("depth"),)
        + (P(None, None, "lat"),) * 2,
        out_specs=by_group,
        check_vma=False,
    )
```

```python
import functools

import jax
import jax.numpy as jnp
from jax import lax
from jax.experimental import pallas as pl
from jax.experimental.pallas import tpu as pltpu
from jax.sharding import PartitionSpec as P

F32 = jnp.float32
BF16 = jnp.bfloat16
MESH = pl.DeviceIdType.MESH
CHUNKS = 4


def halves(value):
    high = value.astype(BF16)
    return high, (value - high.astype(F32)).astype(BF16)


def dot(left, right):
    return lax.dot_general(left, right, (((1,), (0,)), ((), ())), preferred_element_type=F32)


def dot_rows(left, right):
    return lax.dot_general(left, right, (((1,), (1,)), ((), ())), preferred_element_type=F32)


def lanes_of(shape):
    return lax.broadcasted_iota(jnp.int32, shape, 1)


def turn(value):
    n = value.shape[1] // 2
    back = pltpu.roll(value, n, 1)
    return jnp.where(lanes_of(value.shape) < n, -back, back)


def product(left, right):
    l_h, l_l = halves(left)
    r_h, r_l = halves(right)
    out = dot(jnp.concatenate([l_h, l_l], axis=1), jnp.concatenate([r_h, r_h], axis=0))
    return out + dot(l_h, r_l)


def apply(later, offset):
    return product(later[0], jnp.concatenate([offset, turn(offset)], axis=0)) + later[1]


def compose(later, earlier):
    both = jnp.concatenate(earlier, axis=1)
    low = jnp.concatenate([turn(earlier[0]), turn(earlier[1])], axis=1)
    out = product(later[0], jnp.concatenate([both, low], axis=0))
    width = earlier[0].shape[1]
    return out[:, :width], out[:, width:] + later[1]


def select(which, first, second):
    return tuple(jnp.where(which, a, b) for a, b in zip(first, second))


def kernel(
    dims,
    src_hbm, dexp_hbm, dproj_hbm, uexp_hbm, uproj_hbm, ddec_ref, udec_ref, list_ref, count_ref, incd_hbm, incu_hbm,
    out_ref,
    src, exps, inc, pown, near, far, wh, wl, fsend, frecv, ssend, srecv, irecv,
    zsend, zrecv, ysend, yrecv, column, qsend, qrecv,
    load_sem, near_sem, far_send_sem, far_recv_sem, fsend_sem, frecv_sem, ssend_sem, srecv_sem, irecv_sem,
    zsend_sem, zrecv_sem, ysend_sem, yrecv_sem, qsend_sem, qrecv_sem,
):
    ny, nz, nx = dims
    rounds = nz.bit_length() - 1
    masks = [1 << k for k in range(rounds - 1)] + [nz - 1]
    n = src.shape[1]
    size = n // CHUNKS
    width = src.shape[2]
    wide = (n, 2 * n)
    g = lax.axis_index("depth")
    x = lax.axis_index("lat")
    core = lax.rem(g, 2)
    z = lax.rem(lax.div(g, 2), nz)
    y = lax.div(g, 2 * nz)
    mate = g + 1 - 2 * core
    hub = g + 1 - core
    is_hub = core == 1
    sweep = lax.rem(x, 2)
    zz = jnp.where(sweep == 0, z, nz - 1 - z)
    yy = jnp.where(sweep == 0, y, ny - 1 - y)
    begins = jnp.logical_and(yy == 0, zz == 0)
    ends = jnp.logical_and(yy == ny - 1, zz == nz - 1)
    edge = jnp.logical_or(g == 0, g == 2 * ny * nz - 1)
    inner = jnp.logical_not(edge)
    before = jnp.where(edge, g, g - 1 + 2 * core)

    def xor(value, mask):
        out = value
        for bit in range(rounds):
            if mask >> bit & 1:
                out = out + (1 << bit) * (1 - 2 * lax.rem(lax.div(value, 1 << bit), 2))
        return out

    def place(to_y, to_z):
        return (to_y * nz + to_z) * 2 + 1

    z_peers = [place(y, xor(z, mask)) for mask in masks]
    y_peers = [place(jnp.where(sweep == 0, lax.rem(y + o, ny), lax.rem(y + ny - o, ny)), z) for o in range(1, ny)]

    pending = []

    def remote(src_ref, dst_ref, send_sem, recv_sem, to, if_so=None, keep=True):
        copy = pltpu.make_async_remote_copy(
            src_ref=src_ref, dst_ref=dst_ref, send_sem=send_sem, recv_sem=recv_sem,
            device_id=to, device_id_type=MESH,
        )
        if if_so is None:
            copy.start()
        else:
            pl.when(if_so)(copy.start)
        if keep:
            pending.append(copy.wait_send if if_so is None else lambda: pl.when(if_so)(copy.wait_send))
        return copy

    def to_hub(src_ref, dst_ref, send_sem, recv_sem, at, if_so=None):
        itself = jnp.logical_and(is_hub, x == at)
        away = jnp.logical_not(itself)
        if if_so is not None:
            itself, away = jnp.logical_and(itself, if_so), jnp.logical_and(away, if_so)
        copy = remote(src_ref, dst_ref, send_sem, recv_sem, (hub, at), away)
        pl.when(itself)(pltpu.make_async_copy(src_ref, dst_ref, recv_sem).start)
        return copy

    barrier = pltpu.get_barrier_semaphore()

    def greet(group, at):
        pl.semaphore_signal(barrier, inc=1, device_id=(group, at), device_id_type=MESH)

    for o in range(nx):
        greet(mate, lax.rem(x + o, nx))
    pl.when(inner)(lambda: greet(before, x))

    @pl.when(is_hub)
    def _():
        for o in range(1, nx):
            greet(g, lax.rem(x + o, nx))
        for peer in z_peers + y_peers:
            greet(peer, x)

    loads = [
        pltpu.make_async_copy(a, b, load_sem.at[i])
        for i, (a, b) in enumerate(
            [
                (dproj_hbm, pown.at[0]),
                (uproj_hbm, pown.at[1]),
                (dexp_hbm, exps.at[0]),
                (src_hbm, src),
                (uexp_hbm, exps.at[1]),
            ]
        )
    ]
    for copy in loads:
        copy.start()
    inc_copies = [pltpu.make_async_copy(a, inc, load_sem.at[5]) for a in (incd_hbm, incu_hbm)]
    pl.when(jnp.logical_and(edge, core == 0))(inc_copies[0].start)
    pl.when(jnp.logical_and(edge, core == 1))(inc_copies[1].start)

    extra = jnp.where(is_hub, nx - 1 + rounds + ny - 1, 0)
    pl.semaphore_wait(barrier, nx + jnp.where(edge, 0, 1) + extra)

    loads[0].wait()
    loads[1].wait()
    far_copies = []
    for k in range(CHUNKS):
        rows = pl.ds(k * size, size)
        far_copies.append(
            remote(pown.at[core, :, rows], far.at[k], far_send_sem.at[k], far_recv_sem.at[k], (before, x), inner)
        )
        own = pltpu.make_async_copy(pown.at[core, :, rows], far.at[k], far_recv_sem.at[k])
        pl.when(edge)(own.start)
    near_copy = remote(pown.at[1 - core], near, near_sem.at[0], near_sem.at[1], (mate, x))

    square = (n, n)
    row_at = lax.broadcasted_iota(jnp.int32, square, 0)
    lane_at = lanes_of(square)
    valid = jnp.logical_and(list_ref[...] == row_at, lane_at < count_ref[0])
    mask = jnp.sum(jnp.where(valid, 1.0, 0.0), axis=1, keepdims=True)
    for copy in loads[2:]:
        copy.wait()
    for role in range(2):
        first, second = (ddec_ref, udec_ref) if role == 0 else (udec_ref, ddec_ref)
        decay = jnp.where(core == 0, first[...], second[...])
        decay = jnp.sum(jnp.where(row_at == lane_at, decay, 0.0), axis=1, keepdims=True)
        slot = core if role == 0 else 1 - core
        for at in range(2):
            high, low = halves(exps[slot, at] * decay)
            wh[role, pl.ds(at * n, n)] = high
            wl[role, pl.ds(at * n, n)] = low
            high, low = halves(src[at] * mask)
            wh[role, pl.ds((2 + at) * n, n)] = high
            wl[role, pl.ds((2 + at) * n, n)] = low

    @pl.when(edge)
    def _():
        inc_copies[0].wait()
        for at in range(2):
            high, low = halves(inc[at])
            wh[1, pl.ds((2 + at) * n, n)] = high
            wl[1, pl.ds((2 + at) * n, n)] = low

    def meet(right, role):
        rows = right.shape[0] // 2
        p_h, p_l = halves(right)
        both = dot_rows(jnp.concatenate([p_h, p_l], axis=0), wh[role])
        total = both[: 2 * rows] + both[2 * rows :] + dot_rows(p_h, wl[role])
        real, imag = total[:rows], total[rows:]
        return real[:, : 2 * n] + turn(imag[:, : 2 * n]), real[:, 2 * n :] + turn(imag[:, 2 * n :])

    near_copy.wait_recv()
    fsend[0], fsend[1] = meet(near[...].reshape(2 * n, width), 0)
    half = nx // 2
    for j in range(half):
        to_hub(fsend, frecv.at[x], fsend_sem.at[j], frecv_sem.at[x], core + 2 * j)
    for k in range(CHUNKS):
        far_copies[k].wait_recv()
        ssend[k, 0], ssend[k, 1] = meet(far[k].reshape(2 * size, width), 1)
        for j in range(half):
            sem = ssend_sem.at[k, j]
            to_hub(ssend.at[k], srecv.at[k, x], sem, srecv_sem.at[k, x], 1 - core + 2 * j, inner)
            to_hub(ssend.at[k], irecv.at[k, x], sem, irecv_sem.at[k, x], core + 2 * j, edge)

    def arrived(ref, sem):
        pltpu.make_async_copy(ref, ref, sem).wait()

    lane = lanes_of(wide)

    @pl.when(is_hub)
    def _():
        mine = []
        for at in range(nx):
            arrived(frecv.at[at], frecv_sem.at[at])
        for i in range(2):
            total = frecv[0, i]
            for at in range(1, nx):
                total = total + frecv[at, i]
            mine.append(total)
        mine = tuple(mine)

        @pl.when(begins)
        def _():
            totals = []
            for k in range(CHUNKS):
                for at in range(nx):
                    arrived(irecv.at[k, at], irecv_sem.at[k, at])
                total = irecv[k, 0, 1]
                for at in range(1, nx):
                    total = total + irecv[k, at, 1]
                totals.append(total)
            column[0] = jnp.concatenate(totals, axis=0)
            column[1] = apply(mine, column[0])

        first = select(begins, (jnp.zeros(wide, F32), column[1]), mine)

        @pl.when(jnp.logical_not(ends))
        def _():
            parts = [[], []]
            for k in range(CHUNKS):
                for at in range(nx):
                    arrived(srecv.at[k, at], srecv_sem.at[k, at])
                for i in range(2):
                    total = srecv[k, 0, i]
                    for at in range(1, nx):
                        total = total + srecv[k, at, i]
                    parts[i].append(total)
            theirs = tuple(jnp.concatenate(p, axis=0) for p in parts)
            zsend[0, 0], zsend[0, 1] = compose(theirs, first)

        @pl.when(ends)
        def _():
            zsend[0] = jnp.zeros(zsend.shape[1:], F32)

        row = lax.broadcasted_iota(jnp.int32, wide, 0)
        prefix = (jnp.where(row == lane, 1.0, 0.0), jnp.zeros(wide, F32))
        waits = []
        for k in range(rounds):
            copy = remote(
                zsend.at[k], zrecv.at[k], zsend_sem.at[k], zrecv_sem.at[k], (z_peers[k], x), keep=False
            )
            waits.append(copy.wait_send)
            total = (zsend[k, 0], zsend[k, 1])
            copy.wait_recv()
            theirs = (zrecv[k, 0], zrecv[k, 1])
            after = lax.rem(lax.div(zz, 1 << k), 2) == 1
            both = compose(select(after, total, theirs), select(after, theirs, total))
            to = zsend.at[k + 1] if k + 1 < rounds else ysend
            to[0], to[1] = both
            prefix = select(after, compose(prefix, theirs) if k else theirs, prefix)

        y_copies, y_firsts = [], []
        for o in range(1, ny):
            to = (y_peers[o - 1], x)
            sems = (ysend_sem.at[o - 1], yrecv_sem.at[o - 1])
            whole = jnp.logical_and(yy > 0, yy + o < ny)
            y_copies.append(remote(ysend, yrecv.at[o - 1], *sems, to, whole, keep=False))
            y_firsts.append(remote(ysend.at[1], yrecv.at[o - 1, 1], *sems, to, yy == 0, keep=False))
            waits.append(lambda c=y_copies[-1], w=whole: pl.when(w)(c.wait_send))
            waits.append(lambda c=y_firsts[-1]: pl.when(yy == 0)(c.wait_send))

        @pl.when(yy == 0)
        def _():
            qsend[0] = jnp.where(begins, column[0], prefix[1])

        for at in range(1, ny):

            @pl.when(yy == at)
            def _():
                y_firsts[at - 1].wait_recv()
                here = yrecv[at - 1, 1]
                for o in range(at - 1, 0, -1):
                    y_copies[o - 1].wait_recv()
                    here = apply((yrecv[o - 1, 0], yrecv[o - 1, 1]), here)
                qsend[0] = apply(prefix, here)

        beside = x + 1 - 2 * sweep
        chip = g - 1
        for i in range(2):
            if i == 1:
                qsend[1] = apply(mine, qsend[0])
            which = sweep if i == 0 else 1 - sweep
            sems = [(qsend_sem.at[i, j], qrecv_sem.at[sweep]) for j in range(2)]
            copy = remote(qsend.at[i], qrecv.at[sweep], *sems[0], (chip + which, beside), keep=False)
            waits.append(copy.wait_send)
            here = which == 0
            copy = remote(qsend.at[i], qrecv.at[sweep], *sems[1], (chip, x), here, keep=False)
            waits.append(lambda c=copy, w=here: pl.when(w)(c.wait_send))
            own = pltpu.make_async_copy(qsend.at[i], qrecv.at[sweep], qrecv_sem.at[sweep])
            pl.when(which == 1)(own.start)
        for wait in waits:
            wait()

    for at, decay in enumerate((ddec_ref[...], udec_ref[...])):
        arrived(qrecv.at[at], qrecv_sem.at[at])
        columns = qrecv[at]
        turned = jnp.transpose(jnp.concatenate([columns, pltpu.roll(columns, n, 1)], axis=0))[:n]
        out_ref[at] = turned * jnp.concatenate([decay, decay], axis=1)
    for wait in pending:
        wait()


def add_terms(dexp, uexp, src, coef, list_ref, count_ref, out_hbm, field, sems):
    _, n, width = src.shape
    square = (n, n)
    valid = jnp.logical_and(
        list_ref[...] == lax.broadcasted_iota(jnp.int32, square, 0), lanes_of(square) < count_ref[0]
    )
    mask = jnp.sum(jnp.where(valid, 1.0, 0.0), axis=1, keepdims=True)
    parts = []
    for sweep in range(2):
        value = coef[sweep]
        left = lanes_of(value.shape) < n
        parts.append(jnp.concatenate([jnp.where(left, value, -value), pltpu.roll(value, n, 1)], axis=0))
    c_h, c_l = halves(jnp.concatenate(parts, axis=1))
    c_all = jnp.concatenate([c_h, c_l], axis=0)
    step = min(256, width)
    copies = []
    for k in range(width // step):
        cols = pl.ds(k * step, step)
        e_h, e_l = halves(
            jnp.concatenate([dexp[:, :, cols].reshape(2 * n, step), uexp[:, :, cols].reshape(2 * n, step)], axis=0)
        )
        both = dot(c_all, e_h)
        terms = both[: 2 * n] + both[2 * n :] + dot(c_h, e_l)
        for i in range(2):
            field[i, :, cols] = src[i, :, cols] * mask + terms[i * n : (i + 1) * n]
        copies.append(pltpu.make_async_copy(field.at[:, :, cols], out_hbm.at[:, :, cols], sems.at[k]))
        copies[-1].start()
    for copy in copies:
        copy.wait()


def sweeps(dims, *args):
    sources, dexp, dproj, uexp, uproj, ddec, udec, active, count, incd, incu = args
    ny, nz, nx = dims
    _, _, n, width = sources.shape
    size = n // CHUNKS
    rounds = nz.bit_length() - 1
    block = (n, 2 * n)
    hbm = pl.BlockSpec(memory_space=pltpu.HBM)
    vmem = pl.BlockSpec(memory_space=pltpu.VMEM)
    smem = pl.BlockSpec(memory_space=pltpu.SMEM)
    dma = pltpu.SemaphoreType.DMA
    coef = pl.pallas_call(
        functools.partial(kernel, dims),
        out_shape=jax.ShapeDtypeStruct((2, *block), F32),
        in_specs=[hbm] * 5 + [vmem] * 3 + [smem] + [hbm] * 2,
        out_specs=vmem,
        scratch_shapes=[
            pltpu.VMEM((2, n, width), F32),
            pltpu.VMEM((2, 2, n, width), F32),
            pltpu.VMEM((2, n, width), F32),
            pltpu.VMEM((2, 2, n, width), F32),
            pltpu.VMEM((2, n, width), F32),
            pltpu.VMEM((CHUNKS, 2, size, width), F32),
            pltpu.VMEM((2, 4 * n, width), BF16),
            pltpu.VMEM((2, 4 * n, width), BF16),
            pltpu.VMEM((2, *block), F32),
            pltpu.VMEM((nx, 2, *block), F32),
            pltpu.VMEM((CHUNKS, 2, size, 2 * n), F32),
            pltpu.VMEM((CHUNKS, nx, 2, size, 2 * n), F32),
            pltpu.VMEM((CHUNKS, nx, 2, size, 2 * n), F32),
            pltpu.VMEM((rounds, 2, *block), F32),
            pltpu.VMEM((rounds, 2, *block), F32),
            pltpu.VMEM((2, *block), F32),
            pltpu.VMEM((ny - 1, 2, *block), F32),
            pltpu.VMEM((2, *block), F32),
            pltpu.VMEM((2, *block), F32),
            pltpu.VMEM((2, *block), F32),
            dma((6,)),
            dma((2,)),
            dma((CHUNKS,)),
            dma((CHUNKS,)),
            dma((nx // 2,)),
            dma((nx,)),
            dma((CHUNKS, nx // 2)),
            dma((CHUNKS, nx)),
            dma((CHUNKS, nx)),
            dma((rounds,)),
            dma((rounds,)),
            dma((ny - 1,)),
            dma((ny - 1,)),
            dma((2, 2)),
            dma((2,)),
        ],
        compiler_params=pltpu.CompilerParams(
            collective_id=0, has_side_effects=True
        ),
        name="sweeps",
    )(sources[0], dexp[0], dproj[0], uexp[0], uproj[0], ddec, udec, active, count, incd, incu)
    field = pl.pallas_call(
        add_terms,
        out_shape=jax.ShapeDtypeStruct((2, n, width), F32),
        in_specs=[vmem] * 5 + [smem],
        out_specs=hbm,
        scratch_shapes=[pltpu.VMEM((2, n, width), F32), dma((max(1, width // 256),))],

        name="add_terms",
    )(dexp[0], uexp[0], sources[0], coef, active, count)
    return field[None]


def solution(mesh, ny=4):
    depth, nx = mesh.shape["depth"], mesh.shape["lat"]
    dims = (ny, depth // (2 * ny), nx)
    by_group = P("depth", None, None, "lat")
    return jax.shard_map(
        functools.partial(sweeps, dims),
        mesh=mesh,
        in_specs=(by_group,) * 5
        + (P("depth", None),) * 3
        + (P("depth"),)
        + (P(None, None, "lat"),) * 2,
        out_specs=by_group,
        check_vma=False,
    )
```

```python
import functools

import jax
import jax.numpy as jnp
from jax import lax
from jax.experimental import pallas as pl
from jax.experimental.pallas import tpu as pltpu
from jax.sharding import PartitionSpec as P

F32 = jnp.float32
BF16 = jnp.bfloat16
MESH = pl.DeviceIdType.MESH
CHUNKS = 4


def halves(value):
    high = value.astype(BF16)
    return high, (value - high.astype(F32)).astype(BF16)


def dot(left, right):
    return lax.dot_general(left, right, (((1,), (0,)), ((), ())), preferred_element_type=F32)


def dot_rows(left, right):
    return lax.dot_general(left, right, (((1,), (1,)), ((), ())), preferred_element_type=F32)


def lanes_of(shape):
    return lax.broadcasted_iota(jnp.int32, shape, 1)


def turn(value):
    n = value.shape[1] // 2
    back = pltpu.roll(value, n, 1)
    return jnp.where(lanes_of(value.shape) < n, -back, back)


def product(left, right):
    l_h, l_l = halves(left)
    r_h, r_l = halves(right)
    out = dot(jnp.concatenate([l_h, l_l], axis=1), jnp.concatenate([r_h, r_h], axis=0))
    return out + dot(l_h, r_l)


def apply(later, offset):
    return product(later[0], jnp.concatenate([offset, turn(offset)], axis=0)) + later[1]


def compose(later, earlier):
    both = jnp.concatenate(earlier, axis=1)
    low = jnp.concatenate([turn(earlier[0]), turn(earlier[1])], axis=1)
    out = product(later[0], jnp.concatenate([both, low], axis=0))
    width = earlier[0].shape[1]
    return out[:, :width], out[:, width:] + later[1]


def select(which, first, second):
    return tuple(jnp.where(which, a, b) for a, b in zip(first, second))


def kernel(
    dims,
    src_hbm, dexp_hbm, dproj_hbm, uexp_hbm, uproj_hbm, ddec_hbm, udec_hbm, list_hbm, count_ref, incd_hbm, incu_hbm,
    out_ref,
    src, exps, inc, pown, near, far, wh, wl, fsend, frecv, ssend, srecv, irecv,
    zsend, zrecv, ysend, yrecv, column, qsend, qrecv, ddec_ref, udec_ref, list_ref,
    load_sem, near_sem, far_send_sem, far_recv_sem, fsend_sem, frecv_sem, ssend_sem, srecv_sem, irecv_sem,
    zsend_sem, zrecv_sem, ysend_sem, yrecv_sem, qsend_sem, qrecv_sem,
):
    ny, nz, nx = dims
    rounds = nz.bit_length() - 1
    masks = [1 << k for k in range(rounds - 1)] + [nz - 1]
    n = src.shape[1]
    size = n // CHUNKS
    width = src.shape[2]
    wide = (n, 2 * n)
    g = lax.axis_index("depth")
    x = lax.axis_index("lat")
    core = lax.rem(g, 2)
    z = lax.rem(lax.div(g, 2), nz)
    y = lax.div(g, 2 * nz)
    mate = g + 1 - 2 * core
    hub = g + 1 - core
    is_hub = core == 1
    sweep = lax.rem(x, 2)
    zz = jnp.where(sweep == 0, z, nz - 1 - z)
    yy = jnp.where(sweep == 0, y, ny - 1 - y)
    begins = jnp.logical_and(yy == 0, zz == 0)
    ends = jnp.logical_and(yy == ny - 1, zz == nz - 1)
    edge = jnp.logical_or(g == 0, g == 2 * ny * nz - 1)
    inner = jnp.logical_not(edge)
    before = jnp.where(edge, g, g - 1 + 2 * core)

    def xor(value, mask):
        out = value
        for bit in range(rounds):
            if mask >> bit & 1:
                out = out + (1 << bit) * (1 - 2 * lax.rem(lax.div(value, 1 << bit), 2))
        return out

    def place(to_y, to_z):
        return (to_y * nz + to_z) * 2 + 1

    z_peers = [place(y, xor(z, mask)) for mask in masks]
    y_peers = [place(jnp.where(sweep == 0, lax.rem(y + o, ny), lax.rem(y + ny - o, ny)), z) for o in range(1, ny)]

    pending = []

    def remote(src_ref, dst_ref, send_sem, recv_sem, to, if_so=None, keep=True):
        copy = pltpu.make_async_remote_copy(
            src_ref=src_ref, dst_ref=dst_ref, send_sem=send_sem, recv_sem=recv_sem,
            device_id=to, device_id_type=MESH,
        )
        if if_so is None:
            copy.start()
        else:
            pl.when(if_so)(copy.start)
        if keep:
            pending.append(copy.wait_send if if_so is None else lambda: pl.when(if_so)(copy.wait_send))
        return copy

    def to_hub(src_ref, dst_ref, send_sem, recv_sem, at, if_so=None):
        itself = jnp.logical_and(is_hub, x == at)
        away = jnp.logical_not(itself)
        if if_so is not None:
            itself, away = jnp.logical_and(itself, if_so), jnp.logical_and(away, if_so)
        copy = remote(src_ref, dst_ref, send_sem, recv_sem, (hub, at), away)
        pl.when(itself)(pltpu.make_async_copy(src_ref, dst_ref, recv_sem).start)
        return copy

    barrier = pltpu.get_barrier_semaphore()

    def greet(group, at):
        pl.semaphore_signal(barrier, inc=1, device_id=(group, at), device_id_type=MESH)

    for o in range(nx):
        greet(mate, lax.rem(x + o, nx))
    pl.when(inner)(lambda: greet(before, x))

    @pl.when(is_hub)
    def _():
        for o in range(1, nx):
            greet(g, lax.rem(x + o, nx))
        for peer in z_peers + y_peers:
            greet(peer, x)

    loads = [
        pltpu.make_async_copy(a, b, load_sem.at[i])
        for i, (a, b) in enumerate(
            [
                (dproj_hbm, pown.at[0]),
                (uproj_hbm, pown.at[1]),
                (dexp_hbm, exps.at[0]),
                (src_hbm, src),
                (uexp_hbm, exps.at[1]),
                (ddec_hbm, ddec_ref),
                (udec_hbm, udec_ref),
                (list_hbm, list_ref),
            ]
        )
    ]
    for copy in loads:
        copy.start()
    inc_copies = [pltpu.make_async_copy(a, inc, load_sem.at[8]) for a in (incd_hbm, incu_hbm)]
    pl.when(jnp.logical_and(edge, core == 0))(inc_copies[0].start)
    pl.when(jnp.logical_and(edge, core == 1))(inc_copies[1].start)

    extra = jnp.where(is_hub, nx - 1 + rounds + ny - 1, 0)
    pl.semaphore_wait(barrier, nx + jnp.where(edge, 0, 1) + extra)

    loads[0].wait()
    loads[1].wait()
    far_copies = []
    for k in range(CHUNKS):
        rows = pl.ds(k * size, size)
        far_copies.append(
            remote(pown.at[core, :, rows], far.at[k], far_send_sem.at[k], far_recv_sem.at[k], (before, x), inner)
        )
        own = pltpu.make_async_copy(pown.at[core, :, rows], far.at[k], far_recv_sem.at[k])
        pl.when(edge)(own.start)
    near_copy = remote(pown.at[1 - core], near, near_sem.at[0], near_sem.at[1], (mate, x))

    for copy in loads[2:]:
        copy.wait()
    square = (n, n)
    row_at = lax.broadcasted_iota(jnp.int32, square, 0)
    lane_at = lanes_of(square)
    valid = jnp.logical_and(list_ref[...] == row_at, lane_at < count_ref[0])
    mask = jnp.sum(jnp.where(valid, 1.0, 0.0), axis=1, keepdims=True)
    for role in range(2):
        first, second = (ddec_ref, udec_ref) if role == 0 else (udec_ref, ddec_ref)
        decay = jnp.where(core == 0, first[...], second[...])
        decay = jnp.sum(jnp.where(row_at == lane_at, decay, 0.0), axis=1, keepdims=True)
        slot = core if role == 0 else 1 - core
        for at in range(2):
            high, low = halves(exps[slot, at] * decay)
            wh[role, pl.ds(at * n, n)] = high
            wl[role, pl.ds(at * n, n)] = low
            high, low = halves(src[at] * mask)
            wh[role, pl.ds((2 + at) * n, n)] = high
            wl[role, pl.ds((2 + at) * n, n)] = low

    @pl.when(edge)
    def _():
        inc_copies[0].wait()
        for at in range(2):
            high, low = halves(inc[at])
            wh[1, pl.ds((2 + at) * n, n)] = high
            wl[1, pl.ds((2 + at) * n, n)] = low

    def meet(right, role):
        rows = right.shape[0] // 2
        p_h, p_l = halves(right)
        both = dot_rows(jnp.concatenate([p_h, p_l], axis=0), wh[role])
        total = both[: 2 * rows] + both[2 * rows :] + dot_rows(p_h, wl[role])
        real, imag = total[:rows], total[rows:]
        return real[:, : 2 * n] + turn(imag[:, : 2 * n]), real[:, 2 * n :] + turn(imag[:, 2 * n :])

    near_copy.wait_recv()
    fsend[0], fsend[1] = meet(near[...].reshape(2 * n, width), 0)
    half = nx // 2
    for j in range(half):
        to_hub(fsend, frecv.at[x], fsend_sem.at[j], frecv_sem.at[x], core + 2 * j)
    for k in range(CHUNKS):
        far_copies[k].wait_recv()
        ssend[k, 0], ssend[k, 1] = meet(far[k].reshape(2 * size, width), 1)
        for j in range(half):
            sem = ssend_sem.at[k, j]
            to_hub(ssend.at[k], srecv.at[k, x], sem, srecv_sem.at[k, x], 1 - core + 2 * j, inner)
            to_hub(ssend.at[k], irecv.at[k, x], sem, irecv_sem.at[k, x], core + 2 * j, edge)

    def arrived(ref, sem):
        pltpu.make_async_copy(ref, ref, sem).wait()

    lane = lanes_of(wide)

    @pl.when(is_hub)
    def _():
        mine = []
        for at in range(nx):
            arrived(frecv.at[at], frecv_sem.at[at])
        for i in range(2):
            total = frecv[0, i]
            for at in range(1, nx):
                total = total + frecv[at, i]
            mine.append(total)
        mine = tuple(mine)

        @pl.when(begins)
        def _():
            totals = []
            for k in range(CHUNKS):
                for at in range(nx):
                    arrived(irecv.at[k, at], irecv_sem.at[k, at])
                total = irecv[k, 0, 1]
                for at in range(1, nx):
                    total = total + irecv[k, at, 1]
                totals.append(total)
            column[0] = jnp.concatenate(totals, axis=0)
            column[1] = apply(mine, column[0])

        first = select(begins, (jnp.zeros(wide, F32), column[1]), mine)

        @pl.when(jnp.logical_not(ends))
        def _():
            parts = [[], []]
            for k in range(CHUNKS):
                for at in range(nx):
                    arrived(srecv.at[k, at], srecv_sem.at[k, at])
                for i in range(2):
                    total = srecv[k, 0, i]
                    for at in range(1, nx):
                        total = total + srecv[k, at, i]
                    parts[i].append(total)
            theirs = tuple(jnp.concatenate(p, axis=0) for p in parts)
            zsend[0, 0], zsend[0, 1] = compose(theirs, first)

        @pl.when(ends)
        def _():
            zsend[0] = jnp.zeros(zsend.shape[1:], F32)

        row = lax.broadcasted_iota(jnp.int32, wide, 0)
        prefix = (jnp.where(row == lane, 1.0, 0.0), jnp.zeros(wide, F32))
        waits = []
        for k in range(rounds):
            copy = remote(
                zsend.at[k], zrecv.at[k], zsend_sem.at[k], zrecv_sem.at[k], (z_peers[k], x), keep=False
            )
            waits.append(copy.wait_send)
            total = (zsend[k, 0], zsend[k, 1])
            copy.wait_recv()
            theirs = (zrecv[k, 0], zrecv[k, 1])
            after = lax.rem(lax.div(zz, 1 << k), 2) == 1
            both = compose(select(after, total, theirs), select(after, theirs, total))
            to = zsend.at[k + 1] if k + 1 < rounds else ysend
            to[0], to[1] = both
            prefix = select(after, compose(prefix, theirs) if k else theirs, prefix)

        y_copies, y_firsts = [], []
        for o in range(1, ny):
            to = (y_peers[o - 1], x)
            sems = (ysend_sem.at[o - 1], yrecv_sem.at[o - 1])
            whole = jnp.logical_and(yy > 0, yy + o < ny)
            y_copies.append(remote(ysend, yrecv.at[o - 1], *sems, to, whole, keep=False))
            y_firsts.append(remote(ysend.at[1], yrecv.at[o - 1, 1], *sems, to, yy == 0, keep=False))
            waits.append(lambda c=y_copies[-1], w=whole: pl.when(w)(c.wait_send))
            waits.append(lambda c=y_firsts[-1]: pl.when(yy == 0)(c.wait_send))

        @pl.when(yy == 0)
        def _():
            qsend[0] = jnp.where(begins, column[0], prefix[1])

        for at in range(1, ny):

            @pl.when(yy == at)
            def _():
                y_firsts[at - 1].wait_recv()
                here = yrecv[at - 1, 1]
                for o in range(at - 1, 0, -1):
                    y_copies[o - 1].wait_recv()
                    here = apply((yrecv[o - 1, 0], yrecv[o - 1, 1]), here)
                qsend[0] = apply(prefix, here)

        beside = x + 1 - 2 * sweep
        chip = g - 1
        for i in range(2):
            if i == 1:
                qsend[1] = apply(mine, qsend[0])
            which = sweep if i == 0 else 1 - sweep
            sems = [(qsend_sem.at[i, j], qrecv_sem.at[sweep]) for j in range(2)]
            copy = remote(qsend.at[i], qrecv.at[sweep], *sems[0], (chip + which, beside), keep=False)
            waits.append(copy.wait_send)
            here = which == 0
            copy = remote(qsend.at[i], qrecv.at[sweep], *sems[1], (chip, x), here, keep=False)
            waits.append(lambda c=copy, w=here: pl.when(w)(c.wait_send))
            own = pltpu.make_async_copy(qsend.at[i], qrecv.at[sweep], qrecv_sem.at[sweep])
            pl.when(which == 1)(own.start)
        for wait in waits:
            wait()

    for at, decay in enumerate((ddec_ref[...], udec_ref[...])):
        arrived(qrecv.at[at], qrecv_sem.at[at])
        columns = qrecv[at]
        turned = jnp.transpose(jnp.concatenate([columns, pltpu.roll(columns, n, 1)], axis=0))[:n]
        out_ref[at] = turned * jnp.concatenate([decay, decay], axis=1)
    for wait in pending:
        wait()


def add_terms(dexp, uexp, src, coef, list_ref, count_ref, out_hbm, field, sems):
    _, n, width = src.shape
    square = (n, n)
    valid = jnp.logical_and(
        list_ref[...] == lax.broadcasted_iota(jnp.int32, square, 0), lanes_of(square) < count_ref[0]
    )
    mask = jnp.sum(jnp.where(valid, 1.0, 0.0), axis=1, keepdims=True)
    parts = []
    for sweep in range(2):
        value = coef[sweep]
        left = lanes_of(value.shape) < n
        parts.append(jnp.concatenate([jnp.where(left, value, -value), pltpu.roll(value, n, 1)], axis=0))
    c_h, c_l = halves(jnp.concatenate(parts, axis=1))
    c_all = jnp.concatenate([c_h, c_l], axis=0)
    step = min(256, width)
    copies = []
    for k in range(width // step):
        cols = pl.ds(k * step, step)
        e_h, e_l = halves(
            jnp.concatenate([dexp[:, :, cols].reshape(2 * n, step), uexp[:, :, cols].reshape(2 * n, step)], axis=0)
        )
        both = dot(c_all, e_h)
        terms = both[: 2 * n] + both[2 * n :] + dot(c_h, e_l)
        for i in range(2):
            field[i, :, cols] = src[i, :, cols] * mask + terms[i * n : (i + 1) * n]
        copies.append(pltpu.make_async_copy(field.at[:, :, cols], out_hbm.at[:, :, cols], sems.at[k]))
        copies[-1].start()
    for copy in copies:
        copy.wait()


def sweeps(dims, *args):
    sources, dexp, dproj, uexp, uproj, ddec, udec, active, count, incd, incu = args
    ny, nz, nx = dims
    _, _, n, width = sources.shape
    size = n // CHUNKS
    rounds = nz.bit_length() - 1
    block = (n, 2 * n)
    hbm = pl.BlockSpec(memory_space=pltpu.HBM)
    vmem = pl.BlockSpec(memory_space=pltpu.VMEM)
    smem = pl.BlockSpec(memory_space=pltpu.SMEM)
    dma = pltpu.SemaphoreType.DMA
    operands = (sources[0], dexp[0], dproj[0], uexp[0], uproj[0], ddec, udec, active, count, incd, incu)
    coef = pl.pallas_call(
        functools.partial(kernel, dims),
        out_shape=jax.ShapeDtypeStruct((2, *block), F32),
        in_specs=[hbm] * 8 + [smem] + [hbm] * 2,
        out_specs=vmem,
        scratch_shapes=[
            pltpu.VMEM((2, n, width), F32),
            pltpu.VMEM((2, 2, n, width), F32),
            pltpu.VMEM((2, n, width), F32),
            pltpu.VMEM((2, 2, n, width), F32),
            pltpu.VMEM((2, n, width), F32),
            pltpu.VMEM((CHUNKS, 2, size, width), F32),
            pltpu.VMEM((2, 4 * n, width), BF16),
            pltpu.VMEM((2, 4 * n, width), BF16),
            pltpu.VMEM((2, *block), F32),
            pltpu.VMEM((nx, 2, *block), F32),
            pltpu.VMEM((CHUNKS, 2, size, 2 * n), F32),
            pltpu.VMEM((CHUNKS, nx, 2, size, 2 * n), F32),
            pltpu.VMEM((CHUNKS, nx, 2, size, 2 * n), F32),
            pltpu.VMEM((rounds, 2, *block), F32),
            pltpu.VMEM((rounds, 2, *block), F32),
            pltpu.VMEM((2, *block), F32),
            pltpu.VMEM((ny - 1, 2, *block), F32),
            pltpu.VMEM((2, *block), F32),
            pltpu.VMEM((2, *block), F32),
            pltpu.VMEM((2, *block), F32),
            pltpu.VMEM((1, n), F32),
            pltpu.VMEM((1, n), F32),
            pltpu.VMEM((1, n), jnp.int32),
            dma((9,)),
            dma((2,)),
            dma((CHUNKS,)),
            dma((CHUNKS,)),
            dma((nx // 2,)),
            dma((nx,)),
            dma((CHUNKS, nx // 2)),
            dma((CHUNKS, nx)),
            dma((CHUNKS, nx)),
            dma((rounds,)),
            dma((rounds,)),
            dma((ny - 1,)),
            dma((ny - 1,)),
            dma((2, 2)),
            dma((2,)),
        ],
        compiler_params=pltpu.CompilerParams(
            collective_id=0, has_side_effects=True, vmem_limit_bytes=24 * 2**20
        ),
        name="sweeps",
    )(*(v if v is count else pltpu.with_memory_space_constraint(v, pltpu.HBM) for v in operands))
    field = pl.pallas_call(
        add_terms,
        out_shape=jax.ShapeDtypeStruct((2, n, width), F32),
        in_specs=[vmem] * 5 + [smem],
        out_specs=hbm,
        scratch_shapes=[pltpu.VMEM((2, n, width), F32), dma((max(1, width // 256),))],

        compiler_params=pltpu.CompilerParams(vmem_limit_bytes=16 * 2**20),
        name="add_terms",
    )(dexp[0], uexp[0], sources[0], coef, active, count)
    return field[None]


def solution(mesh, ny=4):
    depth, nx = mesh.shape["depth"], mesh.shape["lat"]
    dims = (ny, depth // (2 * ny), nx)
    by_group = P("depth", None, None, "lat")
    return jax.shard_map(
        functools.partial(sweeps, dims),
        mesh=mesh,
        in_specs=(by_group,) * 5
        + (P("depth", None),) * 3
        + (P("depth"),)
        + (P(None, None, "lat"),) * 2,
        out_specs=by_group,
        check_vma=False,
    )
```

```python
import functools

import jax
import jax.numpy as jnp
from jax import lax
from jax.experimental import pallas as pl
from jax.experimental.pallas import tpu as pltpu
from jax.sharding import PartitionSpec as P

F32 = jnp.float32
BF16 = jnp.bfloat16
MESH = pl.DeviceIdType.MESH
CHUNKS = 4


def halves(value):
    high = value.astype(BF16)
    return high, (value - high.astype(F32)).astype(BF16)


def dot(left, right):
    return lax.dot_general(left, right, (((1,), (0,)), ((), ())), preferred_element_type=F32)


def dot_rows(left, right):
    return lax.dot_general(left, right, (((1,), (1,)), ((), ())), preferred_element_type=F32)


def lanes_of(shape):
    return lax.broadcasted_iota(jnp.int32, shape, 1)


def turn(value):
    n = value.shape[1] // 2
    back = pltpu.roll(value, n, 1)
    return jnp.where(lanes_of(value.shape) < n, -back, back)


def product(left, right):
    l_h, l_l = halves(left)
    r_h, r_l = halves(right)
    out = dot(jnp.concatenate([l_h, l_l], axis=1), jnp.concatenate([r_h, r_h], axis=0))
    return out + dot(l_h, r_l)


def apply(later, offset):
    return product(later[0], jnp.concatenate([offset, turn(offset)], axis=0)) + later[1]


def compose(later, earlier):
    both = jnp.concatenate(earlier, axis=1)
    low = jnp.concatenate([turn(earlier[0]), turn(earlier[1])], axis=1)
    out = product(later[0], jnp.concatenate([both, low], axis=0))
    width = earlier[0].shape[1]
    return out[:, :width], out[:, width:] + later[1]


def select(which, first, second):
    return tuple(jnp.where(which, a, b) for a, b in zip(first, second))


def kernel(
    dims,
    src_hbm, dexp_hbm, dproj_hbm, uexp_hbm, uproj_hbm, ddec_hbm, udec_hbm, list_hbm, count_ref, incd_hbm, incu_hbm,
    out_ref,
    src, exps, inc, pown, near, far, wh, wl, fsend, frecv, ssend, srecv, irecv,
    zsend, zrecv, ysend, yrecv, column, qsend, qrecv, ddec_ref, udec_ref, list_ref,
    load_sem, near_sem, far_send_sem, far_recv_sem, fsend_sem, frecv_sem, ssend_sem, srecv_sem, irecv_sem,
    zsend_sem, zrecv_sem, ysend_sem, yrecv_sem, qsend_sem, qrecv_sem,
):
    ny, nz, nx = dims
    rounds = nz.bit_length() - 1
    masks = [1 << k for k in range(rounds - 1)] + [nz - 1]
    n = src.shape[1]
    size = n // CHUNKS
    width = src.shape[2]
    wide = (n, 2 * n)
    g = lax.axis_index("depth")
    x = lax.axis_index("lat")
    core = lax.rem(g, 2)
    z = lax.rem(lax.div(g, 2), nz)
    y = lax.div(g, 2 * nz)
    mate = g + 1 - 2 * core
    hub = g + 1 - core
    is_hub = core == 1
    sweep = lax.rem(x + 1, 2)
    zz = jnp.where(sweep == 0, z, nz - 1 - z)
    yy = jnp.where(sweep == 0, y, ny - 1 - y)
    begins = jnp.logical_and(yy == 0, zz == 0)
    ends = jnp.logical_and(yy == ny - 1, zz == nz - 1)
    edge = jnp.logical_or(g == 0, g == 2 * ny * nz - 1)
    inner = jnp.logical_not(edge)
    before = jnp.where(edge, g, g - 1 + 2 * core)

    def xor(value, mask):
        out = value
        for bit in range(rounds):
            if mask >> bit & 1:
                out = out + (1 << bit) * (1 - 2 * lax.rem(lax.div(value, 1 << bit), 2))
        return out

    def place(to_y, to_z):
        return (to_y * nz + to_z) * 2 + 1

    z_peers = [place(y, xor(z, mask)) for mask in masks]
    y_peers = [place(jnp.where(sweep == 0, lax.rem(y + o, ny), lax.rem(y + ny - o, ny)), z) for o in range(1, ny)]

    pending = []

    def remote(src_ref, dst_ref, send_sem, recv_sem, to, if_so=None, keep=True):
        copy = pltpu.make_async_remote_copy(
            src_ref=src_ref, dst_ref=dst_ref, send_sem=send_sem, recv_sem=recv_sem,
            device_id=to, device_id_type=MESH,
        )
        if if_so is None:
            copy.start()
        else:
            pl.when(if_so)(copy.start)
        if keep:
            pending.append(copy.wait_send if if_so is None else lambda: pl.when(if_so)(copy.wait_send))
        return copy

    def to_hub(src_ref, dst_ref, send_sem, recv_sem, at, if_so=None):
        itself = jnp.logical_and(is_hub, x == at)
        away = jnp.logical_not(itself)
        if if_so is not None:
            itself, away = jnp.logical_and(itself, if_so), jnp.logical_and(away, if_so)
        copy = remote(src_ref, dst_ref, send_sem, recv_sem, (hub, at), away)
        pl.when(itself)(pltpu.make_async_copy(src_ref, dst_ref, recv_sem).start)
        return copy

    barrier = pltpu.get_barrier_semaphore()

    def greet(group, at):
        pl.semaphore_signal(barrier, inc=1, device_id=(group, at), device_id_type=MESH)

    for o in range(nx):
        greet(mate, lax.rem(x + o, nx))
    pl.when(inner)(lambda: greet(before, x))

    @pl.when(is_hub)
    def _():
        for o in range(1, nx):
            greet(g, lax.rem(x + o, nx))
        for peer in z_peers + y_peers:
            greet(peer, x)

    loads = [
        pltpu.make_async_copy(a, b, load_sem.at[i])
        for i, (a, b) in enumerate(
            [
                (dproj_hbm, pown.at[0]),
                (uproj_hbm, pown.at[1]),
                (dexp_hbm, exps.at[0]),
                (src_hbm, src),
                (uexp_hbm, exps.at[1]),
                (ddec_hbm, ddec_ref),
                (udec_hbm, udec_ref),
                (list_hbm, list_ref),
            ]
        )
    ]
    for copy in loads:
        copy.start()
    inc_copies = [pltpu.make_async_copy(a, inc, load_sem.at[8]) for a in (incd_hbm, incu_hbm)]
    pl.when(jnp.logical_and(edge, core == 0))(inc_copies[0].start)
    pl.when(jnp.logical_and(edge, core == 1))(inc_copies[1].start)

    extra = jnp.where(is_hub, nx - 1 + rounds + ny - 1, 0)
    pl.semaphore_wait(barrier, nx + jnp.where(edge, 0, 1) + extra)

    loads[0].wait()
    loads[1].wait()
    far_copies = []
    for k in range(CHUNKS):
        rows = pl.ds(k * size, size)
        far_copies.append(
            remote(pown.at[core, :, rows], far.at[k], far_send_sem.at[k], far_recv_sem.at[k], (before, x), inner)
        )
        own = pltpu.make_async_copy(pown.at[core, :, rows], far.at[k], far_recv_sem.at[k])
        pl.when(edge)(own.start)
    near_copy = remote(pown.at[1 - core], near, near_sem.at[0], near_sem.at[1], (mate, x))

    for copy in loads[2:]:
        copy.wait()
    square = (n, n)
    row_at = lax.broadcasted_iota(jnp.int32, square, 0)
    lane_at = lanes_of(square)
    valid = jnp.logical_and(list_ref[...] == row_at, lane_at < count_ref[0])
    mask = jnp.sum(jnp.where(valid, 1.0, 0.0), axis=1, keepdims=True)
    for role in range(2):
        first, second = (ddec_ref, udec_ref) if role == 0 else (udec_ref, ddec_ref)
        decay = jnp.where(core == 0, first[...], second[...])
        decay = jnp.sum(jnp.where(row_at == lane_at, decay, 0.0), axis=1, keepdims=True)
        slot = core if role == 0 else 1 - core
        for at in range(2):
            high, low = halves(exps[slot, at] * decay)
            wh[role, pl.ds(at * n, n)] = high
            wl[role, pl.ds(at * n, n)] = low
            high, low = halves(src[at] * mask)
            wh[role, pl.ds((2 + at) * n, n)] = high
            wl[role, pl.ds((2 + at) * n, n)] = low

    @pl.when(edge)
    def _():
        inc_copies[0].wait()
        for at in range(2):
            high, low = halves(inc[at])
            wh[1, pl.ds((2 + at) * n, n)] = high
            wl[1, pl.ds((2 + at) * n, n)] = low

    def meet(right, role):
        rows = right.shape[0] // 2
        p_h, p_l = halves(right)
        both = dot_rows(jnp.concatenate([p_h, p_l], axis=0), wh[role])
        total = both[: 2 * rows] + both[2 * rows :] + dot_rows(p_h, wl[role])
        real, imag = total[:rows], total[rows:]
        return real[:, : 2 * n] + turn(imag[:, : 2 * n]), real[:, 2 * n :] + turn(imag[:, 2 * n :])

    near_copy.wait_recv()
    fsend[0], fsend[1] = meet(near[...].reshape(2 * n, width), 0)
    half = nx // 2
    for j in range(half):
        to_hub(fsend, frecv.at[x], fsend_sem.at[j], frecv_sem.at[x], 1 - core + 2 * j)
    for k in range(CHUNKS):
        far_copies[k].wait_recv()
        ssend[k, 0], ssend[k, 1] = meet(far[k].reshape(2 * size, width), 1)
        for j in range(half):
            sem = ssend_sem.at[k, j]
            to_hub(ssend.at[k], srecv.at[k, x], sem, srecv_sem.at[k, x], core + 2 * j, inner)
            to_hub(ssend.at[k], irecv.at[k, x], sem, irecv_sem.at[k, x], 1 - core + 2 * j, edge)

    def arrived(ref, sem):
        pltpu.make_async_copy(ref, ref, sem).wait()

    lane = lanes_of(wide)

    @pl.when(is_hub)
    def _():
        mine = []
        for at in range(nx):
            arrived(frecv.at[at], frecv_sem.at[at])
        for i in range(2):
            total = frecv[0, i]
            for at in range(1, nx):
                total = total + frecv[at, i]
            mine.append(total)
        mine = tuple(mine)

        @pl.when(begins)
        def _():
            totals = []
            for k in range(CHUNKS):
                for at in range(nx):
                    arrived(irecv.at[k, at], irecv_sem.at[k, at])
                total = irecv[k, 0, 1]
                for at in range(1, nx):
                    total = total + irecv[k, at, 1]
                totals.append(total)
            column[0] = jnp.concatenate(totals, axis=0)
            column[1] = apply(mine, column[0])

        first = select(begins, (jnp.zeros(wide, F32), column[1]), mine)

        @pl.when(jnp.logical_not(ends))
        def _():
            parts = [[], []]
            for k in range(CHUNKS):
                for at in range(nx):
                    arrived(srecv.at[k, at], srecv_sem.at[k, at])
                for i in range(2):
                    total = srecv[k, 0, i]
                    for at in range(1, nx):
                        total = total + srecv[k, at, i]
                    parts[i].append(total)
            theirs = tuple(jnp.concatenate(p, axis=0) for p in parts)
            zsend[0, 0], zsend[0, 1] = compose(theirs, first)

        @pl.when(ends)
        def _():
            zsend[0] = jnp.zeros(zsend.shape[1:], F32)

        row = lax.broadcasted_iota(jnp.int32, wide, 0)
        prefix = (jnp.where(row == lane, 1.0, 0.0), jnp.zeros(wide, F32))
        waits = []

        def pass_on(k):
            copy = remote(
                zsend.at[k], zrecv.at[k], zsend_sem.at[k], zrecv_sem.at[k], (z_peers[k], x), keep=False
            )
            waits.append(copy.wait_send)
            return copy

        y_copies, y_firsts = {}, {}

        def pass_down():
            for o in range(ny - 1, 0, -1):
                to = (y_peers[o - 1], x)
                sems = (ysend_sem.at[o - 1], yrecv_sem.at[o - 1])
                whole = jnp.logical_and(yy > 0, yy + o < ny)
                y_copies[o] = remote(ysend, yrecv.at[o - 1], *sems, to, whole, keep=False)
                y_firsts[o] = remote(ysend.at[1], yrecv.at[o - 1, 1], *sems, to, yy == 0, keep=False)
                waits.append(lambda c=y_copies[o], w=whole: pl.when(w)(c.wait_send))
                waits.append(lambda c=y_firsts[o]: pl.when(yy == 0)(c.wait_send))

        copy = pass_on(0)
        for k in range(rounds):
            total = (zsend[k, 0], zsend[k, 1])
            copy.wait_recv()
            theirs = (zrecv[k, 0], zrecv[k, 1])
            after = lax.rem(lax.div(zz, 1 << k), 2) == 1
            both = compose(select(after, total, theirs), select(after, theirs, total))
            if k + 1 < rounds:
                zsend[k + 1, 0], zsend[k + 1, 1] = both
                copy = pass_on(k + 1)
            else:
                ysend[0], ysend[1] = both
                pass_down()
            prefix = select(after, compose(prefix, theirs) if k else theirs, prefix)

        @pl.when(yy == 0)
        def _():
            qsend[0] = jnp.where(begins, column[0], prefix[1])

        for at in range(1, ny):

            @pl.when(yy == at)
            def _():
                last = prefix
                if at > 2:
                    y_copies[1].wait_recv()
                    last = compose(prefix, (yrecv[0, 0], yrecv[0, 1]))
                y_firsts[at].wait_recv()
                here = yrecv[at - 1, 1]
                for o in range(at - 1, 0 if at <= 2 else 1, -1):
                    y_copies[o].wait_recv()
                    here = apply((yrecv[o - 1, 0], yrecv[o - 1, 1]), here)
                qsend[0] = apply(last, here)

        beside = x - 1 + 2 * sweep
        chip = g - 1
        for i in range(2):
            if i == 1:
                qsend[1] = apply(mine, qsend[0])
            which = sweep if i == 0 else 1 - sweep
            sems = [(qsend_sem.at[i, j], qrecv_sem.at[sweep]) for j in range(2)]
            copy = remote(qsend.at[i], qrecv.at[sweep], *sems[0], (chip + which, beside), keep=False)
            waits.append(copy.wait_send)
            here = which == 0
            copy = remote(qsend.at[i], qrecv.at[sweep], *sems[1], (chip, x), here, keep=False)
            waits.append(lambda c=copy, w=here: pl.when(w)(c.wait_send))
            own = pltpu.make_async_copy(qsend.at[i], qrecv.at[sweep], qrecv_sem.at[sweep])
            pl.when(which == 1)(own.start)
        for wait in waits:
            wait()

    for at, decay in enumerate((ddec_ref[...], udec_ref[...])):
        arrived(qrecv.at[at], qrecv_sem.at[at])
        columns = qrecv[at]
        turned = jnp.transpose(jnp.concatenate([columns, pltpu.roll(columns, n, 1)], axis=0))[:n]
        out_ref[at] = turned * jnp.concatenate([decay, decay], axis=1)
    for wait in pending:
        wait()


def add_terms(dexp, uexp, src, coef, list_ref, count_ref, out_hbm, field, sems):
    _, n, width = src.shape
    square = (n, n)
    valid = jnp.logical_and(
        list_ref[...] == lax.broadcasted_iota(jnp.int32, square, 0), lanes_of(square) < count_ref[0]
    )
    mask = jnp.sum(jnp.where(valid, 1.0, 0.0), axis=1, keepdims=True)
    parts = []
    for sweep in range(2):
        value = coef[sweep]
        left = lanes_of(value.shape) < n
        parts.append(jnp.concatenate([jnp.where(left, value, -value), pltpu.roll(value, n, 1)], axis=0))
    c_h, c_l = halves(jnp.concatenate(parts, axis=1))
    c_all = jnp.concatenate([c_h, c_l], axis=0)
    step = min(256, width)
    copies = []
    for k in range(width // step):
        cols = pl.ds(k * step, step)
        e_h, e_l = halves(
            jnp.concatenate([dexp[:, :, cols].reshape(2 * n, step), uexp[:, :, cols].reshape(2 * n, step)], axis=0)
        )
        both = dot(c_all, e_h)
        terms = both[: 2 * n] + both[2 * n :] + dot(c_h, e_l)
        for i in range(2):
            field[i, :, cols] = src[i, :, cols] * mask + terms[i * n : (i + 1) * n]
        copies.append(pltpu.make_async_copy(field.at[:, :, cols], out_hbm.at[:, :, cols], sems.at[k]))
        copies[-1].start()
    for copy in copies:
        copy.wait()


def sweeps(dims, *args):
    sources, dexp, dproj, uexp, uproj, ddec, udec, active, count, incd, incu = args
    ny, nz, nx = dims
    _, _, n, width = sources.shape
    size = n // CHUNKS
    rounds = nz.bit_length() - 1
    block = (n, 2 * n)
    hbm = pl.BlockSpec(memory_space=pltpu.HBM)
    vmem = pl.BlockSpec(memory_space=pltpu.VMEM)
    smem = pl.BlockSpec(memory_space=pltpu.SMEM)
    dma = pltpu.SemaphoreType.DMA
    operands = (sources[0], dexp[0], dproj[0], uexp[0], uproj[0], ddec, udec, active, count, incd, incu)
    coef = pl.pallas_call(
        functools.partial(kernel, dims),
        out_shape=jax.ShapeDtypeStruct((2, *block), F32),
        in_specs=[hbm] * 8 + [smem] + [hbm] * 2,
        out_specs=vmem,
        scratch_shapes=[
            pltpu.VMEM((2, n, width), F32),
            pltpu.VMEM((2, 2, n, width), F32),
            pltpu.VMEM((2, n, width), F32),
            pltpu.VMEM((2, 2, n, width), F32),
            pltpu.VMEM((2, n, width), F32),
            pltpu.VMEM((CHUNKS, 2, size, width), F32),
            pltpu.VMEM((2, 4 * n, width), BF16),
            pltpu.VMEM((2, 4 * n, width), BF16),
            pltpu.VMEM((2, *block), F32),
            pltpu.VMEM((nx, 2, *block), F32),
            pltpu.VMEM((CHUNKS, 2, size, 2 * n), F32),
            pltpu.VMEM((CHUNKS, nx, 2, size, 2 * n), F32),
            pltpu.VMEM((CHUNKS, nx, 2, size, 2 * n), F32),
            pltpu.VMEM((rounds, 2, *block), F32),
            pltpu.VMEM((rounds, 2, *block), F32),
            pltpu.VMEM((2, *block), F32),
            pltpu.VMEM((ny - 1, 2, *block), F32),
            pltpu.VMEM((2, *block), F32),
            pltpu.VMEM((2, *block), F32),
            pltpu.VMEM((2, *block), F32),
            pltpu.VMEM((1, n), F32),
            pltpu.VMEM((1, n), F32),
            pltpu.VMEM((1, n), jnp.int32),
            dma((9,)),
            dma((2,)),
            dma((CHUNKS,)),
            dma((CHUNKS,)),
            dma((nx // 2,)),
            dma((nx,)),
            dma((CHUNKS, nx // 2)),
            dma((CHUNKS, nx)),
            dma((CHUNKS, nx)),
            dma((rounds,)),
            dma((rounds,)),
            dma((ny - 1,)),
            dma((ny - 1,)),
            dma((2, 2)),
            dma((2,)),
        ],
        compiler_params=pltpu.CompilerParams(
            collective_id=0, has_side_effects=True, vmem_limit_bytes=24 * 2**20
        ),
        name="sweeps",
    )(*(v if v is count else pltpu.with_memory_space_constraint(v, pltpu.HBM) for v in operands))
    field = pl.pallas_call(
        add_terms,
        out_shape=jax.ShapeDtypeStruct((2, n, width), F32),
        in_specs=[vmem] * 5 + [smem],
        out_specs=hbm,
        scratch_shapes=[pltpu.VMEM((2, n, width), F32), dma((max(1, width // 256),))],

        compiler_params=pltpu.CompilerParams(vmem_limit_bytes=16 * 2**20),
        name="add_terms",
    )(dexp[0], uexp[0], sources[0], coef, active, count)
    return field[None]


def solution(mesh, ny=4):
    depth, nx = mesh.shape["depth"], mesh.shape["lat"]
    dims = (ny, depth // (2 * ny), nx)
    by_group = P("depth", None, None, "lat")
    return jax.shard_map(
        functools.partial(sweeps, dims),
        mesh=mesh,
        in_specs=(by_group,) * 5
        + (P("depth", None),) * 3
        + (P("depth"),)
        + (P(None, None, "lat"),) * 2,
        out_specs=by_group,
        check_vma=False,
    )
```

```python
import functools

import jax
import jax.numpy as jnp
from jax import lax
from jax.experimental import pallas as pl
from jax.experimental.pallas import tpu as pltpu
from jax.sharding import PartitionSpec as P

F32 = jnp.float32
BF16 = jnp.bfloat16
MESH = pl.DeviceIdType.MESH
CHUNKS = 4


def halves(value):
    high = value.astype(BF16)
    return high, (value - high.astype(F32)).astype(BF16)


def dot(left, right):
    return lax.dot_general(left, right, (((1,), (0,)), ((), ())), preferred_element_type=F32)


def dot_rows(left, right):
    return lax.dot_general(left, right, (((1,), (1,)), ((), ())), preferred_element_type=F32)


def lanes_of(shape):
    return lax.broadcasted_iota(jnp.int32, shape, 1)


def turn(value):
    n = value.shape[1] // 2
    back = pltpu.roll(value, n, 1)
    return jnp.where(lanes_of(value.shape) < n, -back, back)


def product(left, right):
    l_h, l_l = halves(left)
    r_h, r_l = halves(right)
    out = dot(jnp.concatenate([l_h, l_l], axis=1), jnp.concatenate([r_h, r_h], axis=0))
    return out + dot(l_h, r_l)


def apply(later, offset):
    return product(later[0], jnp.concatenate([offset, turn(offset)], axis=0)) + later[1]


def compose(later, earlier):
    both = jnp.concatenate(earlier, axis=1)
    low = jnp.concatenate([turn(earlier[0]), turn(earlier[1])], axis=1)
    out = product(later[0], jnp.concatenate([both, low], axis=0))
    width = earlier[0].shape[1]
    return out[:, :width], out[:, width:] + later[1]


def select(which, first, second):
    return tuple(jnp.where(which, a, b) for a, b in zip(first, second))


def kernel(
    dims,
    src_hbm, dexp_hbm, dproj_hbm, uexp_hbm, uproj_hbm, ddec_hbm, udec_hbm, list_hbm, count_ref, incd_hbm, incu_hbm,
    out_ref,
    src, exps, inc, pown, near, far, wh, wl, fsend, frecv, ssend, srecv, irecv,
    zsend, zrecv, ysend, yrecv, column, qsend, qrecv, ddec_ref, udec_ref, list_ref,
    load_sem, near_sem, far_send_sem, far_recv_sem, fsend_sem, frecv_sem, ssend_sem, srecv_sem, irecv_sem,
    zsend_sem, zrecv_sem, ysend_sem, yrecv_sem, qsend_sem, qrecv_sem,
):
    ny, nz, nx = dims
    rounds = nz.bit_length() - 1
    masks = [(2 << k) - 1 for k in range(rounds)]
    n = src.shape[1]
    size = n // CHUNKS
    width = src.shape[2]
    wide = (n, 2 * n)
    g = lax.axis_index("depth")
    x = lax.axis_index("lat")
    core = lax.rem(g, 2)
    z = lax.rem(lax.div(g, 2), nz)
    y = lax.div(g, 2 * nz)
    mate = g + 1 - 2 * core
    hub = g + 1 - core
    is_hub = core == 1
    sweep = lax.rem(x + 1, 2)
    zz = jnp.where(sweep == 0, z, nz - 1 - z)
    yy = jnp.where(sweep == 0, y, ny - 1 - y)
    begins = jnp.logical_and(yy == 0, zz == 0)
    ends = jnp.logical_and(yy == ny - 1, zz == nz - 1)
    edge = jnp.logical_or(g == 0, g == 2 * ny * nz - 1)
    inner = jnp.logical_not(edge)
    before = jnp.where(edge, g, g - 1 + 2 * core)

    def xor(value, mask):
        out = value
        for bit in range(rounds):
            if mask >> bit & 1:
                out = out + (1 << bit) * (1 - 2 * lax.rem(lax.div(value, 1 << bit), 2))
        return out

    def place(to_y, to_z):
        return (to_y * nz + to_z) * 2 + 1

    z_peers = [place(y, xor(z, mask)) for mask in masks]
    y_peers = [place(jnp.where(sweep == 0, lax.rem(y + o, ny), lax.rem(y + ny - o, ny)), z) for o in range(1, ny)]

    pending = []

    def remote(src_ref, dst_ref, send_sem, recv_sem, to, if_so=None, keep=True):
        copy = pltpu.make_async_remote_copy(
            src_ref=src_ref, dst_ref=dst_ref, send_sem=send_sem, recv_sem=recv_sem,
            device_id=to, device_id_type=MESH,
        )
        if if_so is None:
            copy.start()
        else:
            pl.when(if_so)(copy.start)
        if keep:
            pending.append(copy.wait_send if if_so is None else lambda: pl.when(if_so)(copy.wait_send))
        return copy

    def to_hub(src_ref, dst_ref, send_sem, recv_sem, at, if_so=None):
        itself = jnp.logical_and(is_hub, x == at)
        away = jnp.logical_not(itself)
        if if_so is not None:
            itself, away = jnp.logical_and(itself, if_so), jnp.logical_and(away, if_so)
        copy = remote(src_ref, dst_ref, send_sem, recv_sem, (hub, at), away)
        pl.when(itself)(pltpu.make_async_copy(src_ref, dst_ref, recv_sem).start)
        return copy

    barrier = pltpu.get_barrier_semaphore()

    def greet(group, at):
        pl.semaphore_signal(barrier, inc=1, device_id=(group, at), device_id_type=MESH)

    for o in range(nx):
        greet(mate, lax.rem(x + o, nx))
    pl.when(inner)(lambda: greet(before, x))

    @pl.when(is_hub)
    def _():
        for o in range(1, nx):
            greet(g, lax.rem(x + o, nx))
        for peer in z_peers + y_peers:
            greet(peer, x)

    loads = [
        pltpu.make_async_copy(a, b, load_sem.at[i])
        for i, (a, b) in enumerate(
            [
                (dproj_hbm, pown.at[0]),
                (uproj_hbm, pown.at[1]),
                (dexp_hbm, exps.at[0]),
                (src_hbm, src),
                (uexp_hbm, exps.at[1]),
                (ddec_hbm, ddec_ref),
                (udec_hbm, udec_ref),
                (list_hbm, list_ref),
            ]
        )
    ]
    for copy in loads:
        copy.start()
    inc_copies = [pltpu.make_async_copy(a, inc, load_sem.at[8]) for a in (incd_hbm, incu_hbm)]
    pl.when(jnp.logical_and(edge, core == 0))(inc_copies[0].start)
    pl.when(jnp.logical_and(edge, core == 1))(inc_copies[1].start)

    extra = jnp.where(is_hub, nx - 1 + rounds + ny - 1, 0)
    pl.semaphore_wait(barrier, nx + jnp.where(edge, 0, 1) + extra)

    loads[0].wait()
    loads[1].wait()
    far_copies = []
    for k in range(CHUNKS):
        rows = pl.ds(k * size, size)
        far_copies.append(
            remote(pown.at[core, :, rows], far.at[k], far_send_sem.at[k], far_recv_sem.at[k], (before, x), inner)
        )
        own = pltpu.make_async_copy(pown.at[core, :, rows], far.at[k], far_recv_sem.at[k])
        pl.when(edge)(own.start)
    near_copy = remote(pown.at[1 - core], near, near_sem.at[0], near_sem.at[1], (mate, x))

    for copy in loads[2:]:
        copy.wait()
    square = (n, n)
    row_at = lax.broadcasted_iota(jnp.int32, square, 0)
    lane_at = lanes_of(square)
    valid = jnp.logical_and(list_ref[...] == row_at, lane_at < count_ref[0])
    mask = jnp.sum(jnp.where(valid, 1.0, 0.0), axis=1, keepdims=True)
    for role in range(2):
        first, second = (ddec_ref, udec_ref) if role == 0 else (udec_ref, ddec_ref)
        decay = jnp.where(core == 0, first[...], second[...])
        decay = jnp.sum(jnp.where(row_at == lane_at, decay, 0.0), axis=1, keepdims=True)
        slot = core if role == 0 else 1 - core
        for at in range(2):
            high, low = halves(exps[slot, at] * decay)
            wh[role, pl.ds(at * n, n)] = high
            wl[role, pl.ds(at * n, n)] = low
            high, low = halves(src[at] * mask)
            wh[role, pl.ds((2 + at) * n, n)] = high
            wl[role, pl.ds((2 + at) * n, n)] = low

    @pl.when(edge)
    def _():
        inc_copies[0].wait()
        for at in range(2):
            high, low = halves(inc[at])
            wh[1, pl.ds((2 + at) * n, n)] = high
            wl[1, pl.ds((2 + at) * n, n)] = low

    def meet(right, role):
        rows = right.shape[0] // 2
        p_h, p_l = halves(right)
        both = dot_rows(jnp.concatenate([p_h, p_l], axis=0), wh[role])
        total = both[: 2 * rows] + both[2 * rows :] + dot_rows(p_h, wl[role])
        real, imag = total[:rows], total[rows:]
        return real[:, : 2 * n] + turn(imag[:, : 2 * n]), real[:, 2 * n :] + turn(imag[:, 2 * n :])

    near_copy.wait_recv()
    fsend[0], fsend[1] = meet(near[...].reshape(2 * n, width), 0)
    half = nx // 2
    for j in range(half):
        to_hub(fsend, frecv.at[x], fsend_sem.at[j], frecv_sem.at[x], 1 - core + 2 * j)
    for k in range(CHUNKS):
        far_copies[k].wait_recv()
        ssend[k, 0], ssend[k, 1] = meet(far[k].reshape(2 * size, width), 1)
        for j in range(half):
            sem = ssend_sem.at[k, j]
            to_hub(ssend.at[k], srecv.at[k, x], sem, srecv_sem.at[k, x], core + 2 * j, inner)
            to_hub(ssend.at[k], irecv.at[k, x], sem, irecv_sem.at[k, x], 1 - core + 2 * j, edge)

    def arrived(ref, sem):
        pltpu.make_async_copy(ref, ref, sem).wait()

    lane = lanes_of(wide)

    @pl.when(is_hub)
    def _():
        mine = []
        for at in range(nx):
            arrived(frecv.at[at], frecv_sem.at[at])
        for i in range(2):
            total = frecv[0, i]
            for at in range(1, nx):
                total = total + frecv[at, i]
            mine.append(total)
        mine = tuple(mine)

        @pl.when(begins)
        def _():
            totals = []
            for k in range(CHUNKS):
                for at in range(nx):
                    arrived(irecv.at[k, at], irecv_sem.at[k, at])
                total = irecv[k, 0, 1]
                for at in range(1, nx):
                    total = total + irecv[k, at, 1]
                totals.append(total)
            column[0] = jnp.concatenate(totals, axis=0)
            column[1] = apply(mine, column[0])

        first = select(begins, (jnp.zeros(wide, F32), column[1]), mine)

        @pl.when(jnp.logical_not(ends))
        def _():
            parts = [[], []]
            for k in range(CHUNKS):
                for at in range(nx):
                    arrived(srecv.at[k, at], srecv_sem.at[k, at])
                for i in range(2):
                    total = srecv[k, 0, i]
                    for at in range(1, nx):
                        total = total + srecv[k, at, i]
                    parts[i].append(total)
            theirs = tuple(jnp.concatenate(p, axis=0) for p in parts)
            zsend[0, 0], zsend[0, 1] = compose(theirs, first)

        @pl.when(ends)
        def _():
            zsend[0] = jnp.zeros(zsend.shape[1:], F32)

        row = lax.broadcasted_iota(jnp.int32, wide, 0)
        prefix = (jnp.where(row == lane, 1.0, 0.0), jnp.zeros(wide, F32))
        waits = []

        def pass_on(k):
            copy = remote(
                zsend.at[k], zrecv.at[k], zsend_sem.at[k], zrecv_sem.at[k], (z_peers[k], x), keep=False
            )
            waits.append(copy.wait_send)
            return copy

        y_copies, y_firsts = {}, {}

        def pass_down():
            for o in range(ny - 1, 0, -1):
                to = (y_peers[o - 1], x)
                sems = (ysend_sem.at[o - 1], yrecv_sem.at[o - 1])
                whole = jnp.logical_and(yy > 0, yy + o < ny)
                y_copies[o] = remote(ysend, yrecv.at[o - 1], *sems, to, whole, keep=False)
                y_firsts[o] = remote(ysend.at[1], yrecv.at[o - 1, 1], *sems, to, yy == 0, keep=False)
                waits.append(lambda c=y_copies[o], w=whole: pl.when(w)(c.wait_send))
                waits.append(lambda c=y_firsts[o]: pl.when(yy == 0)(c.wait_send))

        copy = pass_on(0)
        for k in range(rounds):
            total = (zsend[k, 0], zsend[k, 1])
            copy.wait_recv()
            theirs = (zrecv[k, 0], zrecv[k, 1])
            after = lax.rem(lax.div(zz, 1 << k), 2) == 1
            both = compose(select(after, total, theirs), select(after, theirs, total))
            if k + 1 < rounds:
                zsend[k + 1, 0], zsend[k + 1, 1] = both
                copy = pass_on(k + 1)
            else:
                ysend[0], ysend[1] = both
                pass_down()
            prefix = select(after, compose(prefix, theirs) if k else theirs, prefix)

        @pl.when(yy == 0)
        def _():
            qsend[0] = jnp.where(begins, column[0], prefix[1])

        for at in range(1, ny):

            @pl.when(yy == at)
            def _():
                last = prefix
                if at > 2:
                    y_copies[1].wait_recv()
                    last = compose(prefix, (yrecv[0, 0], yrecv[0, 1]))
                y_firsts[at].wait_recv()
                here = yrecv[at - 1, 1]
                for o in range(at - 1, 0 if at <= 2 else 1, -1):
                    y_copies[o].wait_recv()
                    here = apply((yrecv[o - 1, 0], yrecv[o - 1, 1]), here)
                qsend[0] = apply(last, here)

        beside = x - 1 + 2 * sweep
        chip = g - 1
        for i in range(2):
            if i == 1:
                qsend[1] = apply(mine, qsend[0])
            which = sweep if i == 0 else 1 - sweep
            sems = [(qsend_sem.at[i, j], qrecv_sem.at[sweep]) for j in range(2)]
            copy = remote(qsend.at[i], qrecv.at[sweep], *sems[0], (chip + which, beside), keep=False)
            waits.append(copy.wait_send)
            here = which == 0
            copy = remote(qsend.at[i], qrecv.at[sweep], *sems[1], (chip, x), here, keep=False)
            waits.append(lambda c=copy, w=here: pl.when(w)(c.wait_send))
            own = pltpu.make_async_copy(qsend.at[i], qrecv.at[sweep], qrecv_sem.at[sweep])
            pl.when(which == 1)(own.start)
        for wait in waits:
            wait()

    for at, decay in enumerate((ddec_ref[...], udec_ref[...])):
        arrived(qrecv.at[at], qrecv_sem.at[at])
        columns = qrecv[at]
        turned = jnp.transpose(jnp.concatenate([columns, pltpu.roll(columns, n, 1)], axis=0))[:n]
        out_ref[at] = turned * jnp.concatenate([decay, decay], axis=1)
    for wait in pending:
        wait()


def add_terms(dexp, uexp, src, coef, list_ref, count_ref, out_hbm, field, sems):
    _, n, width = src.shape
    square = (n, n)
    valid = jnp.logical_and(
        list_ref[...] == lax.broadcasted_iota(jnp.int32, square, 0), lanes_of(square) < count_ref[0]
    )
    mask = jnp.sum(jnp.where(valid, 1.0, 0.0), axis=1, keepdims=True)
    parts = []
    for sweep in range(2):
        value = coef[sweep]
        left = lanes_of(value.shape) < n
        parts.append(jnp.concatenate([jnp.where(left, value, -value), pltpu.roll(value, n, 1)], axis=0))
    c_h, c_l = halves(jnp.concatenate(parts, axis=1))
    c_all = jnp.concatenate([c_h, c_l], axis=0)
    step = min(256, width)
    copies = []
    for k in range(width // step):
        cols = pl.ds(k * step, step)
        e_h, e_l = halves(
            jnp.concatenate([dexp[:, :, cols].reshape(2 * n, step), uexp[:, :, cols].reshape(2 * n, step)], axis=0)
        )
        both = dot(c_all, e_h)
        terms = both[: 2 * n] + both[2 * n :] + dot(c_h, e_l)
        for i in range(2):
            field[i, :, cols] = src[i, :, cols] * mask + terms[i * n : (i + 1) * n]
        copies.append(pltpu.make_async_copy(field.at[:, :, cols], out_hbm.at[:, :, cols], sems.at[k]))
        copies[-1].start()
    for copy in copies:
        copy.wait()


def sweeps(dims, *args):
    sources, dexp, dproj, uexp, uproj, ddec, udec, active, count, incd, incu = args
    ny, nz, nx = dims
    _, _, n, width = sources.shape
    size = n // CHUNKS
    rounds = nz.bit_length() - 1
    block = (n, 2 * n)
    hbm = pl.BlockSpec(memory_space=pltpu.HBM)
    vmem = pl.BlockSpec(memory_space=pltpu.VMEM)
    smem = pl.BlockSpec(memory_space=pltpu.SMEM)
    dma = pltpu.SemaphoreType.DMA
    operands = (sources[0], dexp[0], dproj[0], uexp[0], uproj[0], ddec, udec, active, count, incd, incu)
    coef = pl.pallas_call(
        functools.partial(kernel, dims),
        out_shape=jax.ShapeDtypeStruct((2, *block), F32),
        in_specs=[hbm] * 8 + [smem] + [hbm] * 2,
        out_specs=vmem,
        scratch_shapes=[
            pltpu.VMEM((2, n, width), F32),
            pltpu.VMEM((2, 2, n, width), F32),
            pltpu.VMEM((2, n, width), F32),
            pltpu.VMEM((2, 2, n, width), F32),
            pltpu.VMEM((2, n, width), F32),
            pltpu.VMEM((CHUNKS, 2, size, width), F32),
            pltpu.VMEM((2, 4 * n, width), BF16),
            pltpu.VMEM((2, 4 * n, width), BF16),
            pltpu.VMEM((2, *block), F32),
            pltpu.VMEM((nx, 2, *block), F32),
            pltpu.VMEM((CHUNKS, 2, size, 2 * n), F32),
            pltpu.VMEM((CHUNKS, nx, 2, size, 2 * n), F32),
            pltpu.VMEM((CHUNKS, nx, 2, size, 2 * n), F32),
            pltpu.VMEM((rounds, 2, *block), F32),
            pltpu.VMEM((rounds, 2, *block), F32),
            pltpu.VMEM((2, *block), F32),
            pltpu.VMEM((ny - 1, 2, *block), F32),
            pltpu.VMEM((2, *block), F32),
            pltpu.VMEM((2, *block), F32),
            pltpu.VMEM((2, *block), F32),
            pltpu.VMEM((1, n), F32),
            pltpu.VMEM((1, n), F32),
            pltpu.VMEM((1, n), jnp.int32),
            dma((9,)),
            dma((2,)),
            dma((CHUNKS,)),
            dma((CHUNKS,)),
            dma((nx // 2,)),
            dma((nx,)),
            dma((CHUNKS, nx // 2)),
            dma((CHUNKS, nx)),
            dma((CHUNKS, nx)),
            dma((rounds,)),
            dma((rounds,)),
            dma((ny - 1,)),
            dma((ny - 1,)),
            dma((2, 2)),
            dma((2,)),
        ],
        compiler_params=pltpu.CompilerParams(
            collective_id=0, has_side_effects=True, vmem_limit_bytes=24 * 2**20
        ),
        name="sweeps",
    )(*(v if v is count else pltpu.with_memory_space_constraint(v, pltpu.HBM) for v in operands))
    field = pl.pallas_call(
        add_terms,
        out_shape=jax.ShapeDtypeStruct((2, n, width), F32),
        in_specs=[vmem] * 5 + [smem],
        out_specs=hbm,
        scratch_shapes=[pltpu.VMEM((2, n, width), F32), dma((max(1, width // 256),))],

        compiler_params=pltpu.CompilerParams(vmem_limit_bytes=16 * 2**20),
        name="add_terms",
    )(dexp[0], uexp[0], sources[0], coef, active, count)
    return field[None]


def solution(mesh, ny=4):
    depth, nx = mesh.shape["depth"], mesh.shape["lat"]
    dims = (ny, depth // (2 * ny), nx)
    by_group = P("depth", None, None, "lat")
    return jax.shard_map(
        functools.partial(sweeps, dims),
        mesh=mesh,
        in_specs=(by_group,) * 5
        + (P("depth", None),) * 3
        + (P("depth"),)
        + (P(None, None, "lat"),) * 2,
        out_specs=by_group,
        check_vma=False,
    )
```

```python
import functools

import jax
import jax.numpy as jnp
from jax import lax
from jax.experimental import pallas as pl
from jax.experimental.pallas import tpu as pltpu
from jax.sharding import PartitionSpec as P

F32 = jnp.float32
BF16 = jnp.bfloat16
MESH = pl.DeviceIdType.MESH
CHUNKS = 4


def halves(value):
    high = value.astype(BF16)
    return high, (value - high.astype(F32)).astype(BF16)


def dot(left, right):
    return lax.dot_general(left, right, (((1,), (0,)), ((), ())), preferred_element_type=F32)


def dot_rows(left, right):
    return lax.dot_general(left, right, (((1,), (1,)), ((), ())), preferred_element_type=F32)


def lanes_of(shape):
    return lax.broadcasted_iota(jnp.int32, shape, 1)


def turn(value):
    n = value.shape[1] // 2
    back = pltpu.roll(value, n, 1)
    return jnp.where(lanes_of(value.shape) < n, -back, back)


def product(left, right):
    l_h, l_l = halves(left)
    r_h, r_l = halves(right)
    out = dot(jnp.concatenate([l_h, l_l], axis=1), jnp.concatenate([r_h, r_h], axis=0))
    return out + dot(l_h, r_l)


def apply(later, offset):
    return product(later[0], jnp.concatenate([offset, turn(offset)], axis=0)) + later[1]


def compose(later, earlier):
    both = jnp.concatenate(earlier, axis=1)
    low = jnp.concatenate([turn(earlier[0]), turn(earlier[1])], axis=1)
    out = product(later[0], jnp.concatenate([both, low], axis=0))
    width = earlier[0].shape[1]
    return out[:, :width], out[:, width:] + later[1]


def select(which, first, second):
    return tuple(jnp.where(which, a, b) for a, b in zip(first, second))


def kernel(
    dims,
    src_hbm, dexp_hbm, dproj_hbm, uexp_hbm, uproj_hbm, ddec_hbm, udec_hbm, list_hbm, count_ref, incd_hbm, incu_hbm,
    out_ref,
    src, exps, inc, pown, near, far, wh, wl, fsend, frecv, ssend, srecv, irecv,
    zsend, zrecv, ysend, yrecv, column, qsend, qrecv, ddec_ref, udec_ref, list_ref,
    load_sem, near_sem, far_send_sem, far_recv_sem, fsend_sem, frecv_sem, ssend_sem, srecv_sem, irecv_sem,
    zsend_sem, zrecv_sem, ysend_sem, yrecv_sem, qsend_sem, qrecv_sem,
):
    ny, nz, nx = dims
    rounds = nz.bit_length() - 1
    masks = [(2 << k) - 1 for k in range(rounds)]
    n = src.shape[1]
    size = n // CHUNKS
    width = src.shape[2]
    wide = (n, 2 * n)
    g = lax.axis_index("depth")
    x = lax.axis_index("lat")
    core = lax.rem(g, 2)
    z = lax.rem(lax.div(g, 2), nz)
    y = lax.div(g, 2 * nz)
    mate = g + 1 - 2 * core
    hub = g + 1 - core
    is_hub = core == 1
    sweep = lax.rem(x + 1, 2)
    zz = jnp.where(sweep == 0, z, nz - 1 - z)
    yy = jnp.where(sweep == 0, y, ny - 1 - y)
    begins = jnp.logical_and(yy == 0, zz == 0)
    ends = jnp.logical_and(yy == ny - 1, zz == nz - 1)
    edge = jnp.logical_or(g == 0, g == 2 * ny * nz - 1)
    inner = jnp.logical_not(edge)
    before = jnp.where(edge, g, g - 1 + 2 * core)

    def xor(value, mask):
        out = value
        for bit in range(rounds):
            if mask >> bit & 1:
                out = out + (1 << bit) * (1 - 2 * lax.rem(lax.div(value, 1 << bit), 2))
        return out

    def place(to_y, to_z):
        return (to_y * nz + to_z) * 2 + 1

    z_peers = [place(y, xor(z, mask)) for mask in masks]
    y_peers = [place(jnp.where(sweep == 0, lax.rem(y + o, ny), lax.rem(y + ny - o, ny)), z) for o in range(1, ny)]

    pending = []

    def remote(src_ref, dst_ref, send_sem, recv_sem, to, if_so=None, keep=True):
        copy = pltpu.make_async_remote_copy(
            src_ref=src_ref, dst_ref=dst_ref, send_sem=send_sem, recv_sem=recv_sem,
            device_id=to, device_id_type=MESH,
        )
        if if_so is None:
            copy.start()
        else:
            pl.when(if_so)(copy.start)
        if keep:
            pending.append(copy.wait_send if if_so is None else lambda: pl.when(if_so)(copy.wait_send))
        return copy

    def to_hub(src_ref, dst_ref, send_sem, recv_sem, at, if_so=None):
        itself = jnp.logical_and(is_hub, x == at)
        away = jnp.logical_not(itself)
        if if_so is not None:
            itself, away = jnp.logical_and(itself, if_so), jnp.logical_and(away, if_so)
        copy = remote(src_ref, dst_ref, send_sem, recv_sem, (hub, at), away)
        pl.when(itself)(pltpu.make_async_copy(src_ref, dst_ref, recv_sem).start)
        return copy

    barrier = pltpu.get_barrier_semaphore()

    def greet(group, at):
        pl.semaphore_signal(barrier, inc=1, device_id=(group, at), device_id_type=MESH)

    for o in range(nx):
        greet(mate, lax.rem(x + o, nx))
    pl.when(inner)(lambda: greet(before, x))

    @pl.when(is_hub)
    def _():
        for o in range(1, nx):
            greet(g, lax.rem(x + o, nx))
        for peer in z_peers + y_peers:
            greet(peer, x)

    loads = [
        pltpu.make_async_copy(a, b, load_sem.at[i])
        for i, (a, b) in enumerate(
            [
                (dproj_hbm, pown.at[0]),
                (uproj_hbm, pown.at[1]),
                (dexp_hbm, exps.at[0]),
                (src_hbm, src),
                (uexp_hbm, exps.at[1]),
                (ddec_hbm, ddec_ref),
                (udec_hbm, udec_ref),
                (list_hbm, list_ref),
            ]
        )
    ]
    for copy in loads:
        copy.start()
    inc_copies = [pltpu.make_async_copy(a, inc, load_sem.at[8]) for a in (incd_hbm, incu_hbm)]
    pl.when(jnp.logical_and(edge, core == 0))(inc_copies[0].start)
    pl.when(jnp.logical_and(edge, core == 1))(inc_copies[1].start)

    extra = jnp.where(is_hub, nx - 1 + rounds + ny - 1, 0)
    pl.semaphore_wait(barrier, nx + jnp.where(edge, 0, 1) + extra)

    loads[0].wait()
    loads[1].wait()
    far_copies = []
    for k in range(CHUNKS):
        rows = pl.ds(k * size, size)
        far_copies.append(
            remote(pown.at[core, :, rows], far.at[k], far_send_sem.at[k], far_recv_sem.at[k], (before, x), inner)
        )
        own = pltpu.make_async_copy(pown.at[core, :, rows], far.at[k], far_recv_sem.at[k])
        pl.when(edge)(own.start)
    near_copy = remote(pown.at[1 - core], near, near_sem.at[0], near_sem.at[1], (mate, x))

    for copy in loads[2:]:
        copy.wait()
    square = (n, n)
    row_at = lax.broadcasted_iota(jnp.int32, square, 0)
    lane_at = lanes_of(square)
    valid = jnp.logical_and(list_ref[...] == row_at, lane_at < count_ref[0])
    mask = jnp.sum(jnp.where(valid, 1.0, 0.0), axis=1, keepdims=True)
    for role in range(2):
        first, second = (ddec_ref, udec_ref) if role == 0 else (udec_ref, ddec_ref)
        decay = jnp.where(core == 0, first[...], second[...])
        decay = jnp.sum(jnp.where(row_at == lane_at, decay, 0.0), axis=1, keepdims=True)
        slot = core if role == 0 else 1 - core
        for at in range(2):
            high, low = halves(exps[slot, at] * decay)
            wh[role, pl.ds(at * n, n)] = high
            wl[role, pl.ds(at * n, n)] = low
            high, low = halves(src[at] * mask)
            wh[role, pl.ds((2 + at) * n, n)] = high
            wl[role, pl.ds((2 + at) * n, n)] = low

    @pl.when(edge)
    def _():
        inc_copies[0].wait()
        for at in range(2):
            high, low = halves(inc[at])
            wh[1, pl.ds((2 + at) * n, n)] = high
            wl[1, pl.ds((2 + at) * n, n)] = low

    def meet(right, role):
        rows = right.shape[0] // 2
        p_h, p_l = halves(right)
        both = dot_rows(jnp.concatenate([p_h, p_l], axis=0), wh[role])
        total = both[: 2 * rows] + both[2 * rows :] + dot_rows(p_h, wl[role])
        real, imag = total[:rows], total[rows:]
        return real[:, : 2 * n] + turn(imag[:, : 2 * n]), real[:, 2 * n :] + turn(imag[:, 2 * n :])

    near_copy.wait_recv()
    fsend[0], fsend[1] = meet(near[...].reshape(2 * n, width), 0)
    half = nx // 2
    for j in range(half):
        to_hub(fsend, frecv.at[x], fsend_sem.at[j], frecv_sem.at[x], 1 - core + 2 * j)
    for k in range(CHUNKS):
        far_copies[k].wait_recv()
        ssend[k, 0], ssend[k, 1] = meet(far[k].reshape(2 * size, width), 1)
        for j in range(half):
            sem = ssend_sem.at[k, j]
            to_hub(ssend.at[k], srecv.at[k, x], sem, srecv_sem.at[k, x], core + 2 * j, inner)
            to_hub(ssend.at[k], irecv.at[k, x], sem, irecv_sem.at[k, x], 1 - core + 2 * j, edge)

    def arrived(ref, sem):
        pltpu.make_async_copy(ref, ref, sem).wait()

    def hand_over():
        for at, decay in enumerate((ddec_ref[...], udec_ref[...])):
            arrived(qrecv.at[at], qrecv_sem.at[at])
            columns = qrecv[at]
            turned = jnp.transpose(jnp.concatenate([columns, pltpu.roll(columns, n, 1)], axis=0))[:n]
            out_ref[at] = turned * jnp.concatenate([decay, decay], axis=1)

    lane = lanes_of(wide)

    @pl.when(is_hub)
    def _():
        mine = []
        for at in range(nx):
            arrived(frecv.at[at], frecv_sem.at[at])
        for i in range(2):
            total = frecv[0, i]
            for at in range(1, nx):
                total = total + frecv[at, i]
            mine.append(total)
        mine = tuple(mine)

        @pl.when(begins)
        def _():
            totals = []
            for k in range(CHUNKS):
                for at in range(nx):
                    arrived(irecv.at[k, at], irecv_sem.at[k, at])
                total = irecv[k, 0, 1]
                for at in range(1, nx):
                    total = total + irecv[k, at, 1]
                totals.append(total)
            column[0] = jnp.concatenate(totals, axis=0)
            column[1] = apply(mine, column[0])

        first = select(begins, (jnp.zeros(wide, F32), column[1]), mine)

        @pl.when(jnp.logical_not(ends))
        def _():
            parts = [[], []]
            for k in range(CHUNKS):
                for at in range(nx):
                    arrived(srecv.at[k, at], srecv_sem.at[k, at])
                for i in range(2):
                    total = srecv[k, 0, i]
                    for at in range(1, nx):
                        total = total + srecv[k, at, i]
                    parts[i].append(total)
            theirs = tuple(jnp.concatenate(p, axis=0) for p in parts)
            zsend[0, 0], zsend[0, 1] = compose(theirs, first)

        @pl.when(ends)
        def _():
            zsend[0] = jnp.zeros(zsend.shape[1:], F32)

        row = lax.broadcasted_iota(jnp.int32, wide, 0)
        prefix = (jnp.where(row == lane, 1.0, 0.0), jnp.zeros(wide, F32))
        waits = []

        def pass_on(k):
            copy = remote(
                zsend.at[k], zrecv.at[k], zsend_sem.at[k], zrecv_sem.at[k], (z_peers[k], x), keep=False
            )
            waits.append(copy.wait_send)
            return copy

        y_copies, y_firsts = {}, {}

        def pass_down():
            for o in range(ny - 1, 0, -1):
                to = (y_peers[o - 1], x)
                sems = (ysend_sem.at[o - 1], yrecv_sem.at[o - 1])
                whole = jnp.logical_and(yy > 0, yy + o < ny)
                y_copies[o] = remote(ysend, yrecv.at[o - 1], *sems, to, whole, keep=False)
                y_firsts[o] = remote(ysend.at[1], yrecv.at[o - 1, 1], *sems, to, yy == 0, keep=False)
                waits.append(lambda c=y_copies[o], w=whole: pl.when(w)(c.wait_send))
                waits.append(lambda c=y_firsts[o]: pl.when(yy == 0)(c.wait_send))

        copy = pass_on(0)
        for k in range(rounds):
            total = (zsend[k, 0], zsend[k, 1])
            copy.wait_recv()
            theirs = (zrecv[k, 0], zrecv[k, 1])
            after = lax.rem(lax.div(zz, 1 << k), 2) == 1
            both = compose(select(after, total, theirs), select(after, theirs, total))
            if k + 1 < rounds:
                zsend[k + 1, 0], zsend[k + 1, 1] = both
                copy = pass_on(k + 1)
            else:
                ysend[0], ysend[1] = both
                pass_down()
            prefix = select(after, compose(prefix, theirs) if k else theirs, prefix)

        @pl.when(yy == 0)
        def _():
            qsend[0] = jnp.where(begins, column[0], prefix[1])

        for at in range(1, ny):

            @pl.when(yy == at)
            def _():
                last = prefix
                if at > 2:
                    y_copies[1].wait_recv()
                    last = compose(prefix, (yrecv[0, 0], yrecv[0, 1]))
                y_firsts[at].wait_recv()
                here = yrecv[at - 1, 1]
                for o in range(at - 1, 0 if at <= 2 else 1, -1):
                    y_copies[o].wait_recv()
                    here = apply((yrecv[o - 1, 0], yrecv[o - 1, 1]), here)
                qsend[0] = apply(last, here)

        beside = x - 1 + 2 * sweep
        chip = g - 1
        for i in range(2):
            if i == 1:
                qsend[1] = apply(mine, qsend[0])
            which = sweep if i == 0 else 1 - sweep
            sems = [(qsend_sem.at[i, j], qrecv_sem.at[sweep]) for j in range(2)]
            copy = remote(qsend.at[i], qrecv.at[sweep], *sems[0], (chip + which, beside), keep=False)
            waits.append(copy.wait_send)
            here = which == 0
            copy = remote(qsend.at[i], qrecv.at[sweep], *sems[1], (chip, x), here, keep=False)
            waits.append(lambda c=copy, w=here: pl.when(w)(c.wait_send))
            own = pltpu.make_async_copy(qsend.at[i], qrecv.at[sweep], qrecv_sem.at[sweep])
            pl.when(which == 1)(own.start)
        hand_over()
        for wait in waits:
            wait()

    pl.when(jnp.logical_not(is_hub))(hand_over)
    for wait in pending:
        wait()


def add_terms(dexp, uexp, src, coef, list_ref, count_ref, out_hbm, field, sems):
    _, n, width = src.shape
    square = (n, n)
    valid = jnp.logical_and(
        list_ref[...] == lax.broadcasted_iota(jnp.int32, square, 0), lanes_of(square) < count_ref[0]
    )
    mask = jnp.sum(jnp.where(valid, 1.0, 0.0), axis=1, keepdims=True)
    parts = []
    for sweep in range(2):
        value = coef[sweep]
        left = lanes_of(value.shape) < n
        parts.append(jnp.concatenate([jnp.where(left, value, -value), pltpu.roll(value, n, 1)], axis=0))
    c_h, c_l = halves(jnp.concatenate(parts, axis=1))
    c_all = jnp.concatenate([c_h, c_l], axis=0)
    step = min(256, width)
    copies = []
    for k in range(width // step):
        cols = pl.ds(k * step, step)
        e_h, e_l = halves(
            jnp.concatenate([dexp[:, :, cols].reshape(2 * n, step), uexp[:, :, cols].reshape(2 * n, step)], axis=0)
        )
        both = dot(c_all, e_h)
        terms = both[: 2 * n] + both[2 * n :] + dot(c_h, e_l)
        for i in range(2):
            field[i, :, cols] = src[i, :, cols] * mask + terms[i * n : (i + 1) * n]
        copies.append(pltpu.make_async_copy(field.at[:, :, cols], out_hbm.at[:, :, cols], sems.at[k]))
        copies[-1].start()
    for copy in copies:
        copy.wait()


def sweeps(dims, *args):
    sources, dexp, dproj, uexp, uproj, ddec, udec, active, count, incd, incu = args
    ny, nz, nx = dims
    _, _, n, width = sources.shape
    size = n // CHUNKS
    rounds = nz.bit_length() - 1
    block = (n, 2 * n)
    hbm = pl.BlockSpec(memory_space=pltpu.HBM)
    vmem = pl.BlockSpec(memory_space=pltpu.VMEM)
    smem = pl.BlockSpec(memory_space=pltpu.SMEM)
    dma = pltpu.SemaphoreType.DMA
    operands = (sources[0], dexp[0], dproj[0], uexp[0], uproj[0], ddec, udec, active, count, incd, incu)
    coef = pl.pallas_call(
        functools.partial(kernel, dims),
        out_shape=jax.ShapeDtypeStruct((2, *block), F32),
        in_specs=[hbm] * 8 + [smem] + [hbm] * 2,
        out_specs=vmem,
        scratch_shapes=[
            pltpu.VMEM((2, n, width), F32),
            pltpu.VMEM((2, 2, n, width), F32),
            pltpu.VMEM((2, n, width), F32),
            pltpu.VMEM((2, 2, n, width), F32),
            pltpu.VMEM((2, n, width), F32),
            pltpu.VMEM((CHUNKS, 2, size, width), F32),
            pltpu.VMEM((2, 4 * n, width), BF16),
            pltpu.VMEM((2, 4 * n, width), BF16),
            pltpu.VMEM((2, *block), F32),
            pltpu.VMEM((nx, 2, *block), F32),
            pltpu.VMEM((CHUNKS, 2, size, 2 * n), F32),
            pltpu.VMEM((CHUNKS, nx, 2, size, 2 * n), F32),
            pltpu.VMEM((CHUNKS, nx, 2, size, 2 * n), F32),
            pltpu.VMEM((rounds, 2, *block), F32),
            pltpu.VMEM((rounds, 2, *block), F32),
            pltpu.VMEM((2, *block), F32),
            pltpu.VMEM((ny - 1, 2, *block), F32),
            pltpu.VMEM((2, *block), F32),
            pltpu.VMEM((2, *block), F32),
            pltpu.VMEM((2, *block), F32),
            pltpu.VMEM((1, n), F32),
            pltpu.VMEM((1, n), F32),
            pltpu.VMEM((1, n), jnp.int32),
            dma((9,)),
            dma((2,)),
            dma((CHUNKS,)),
            dma((CHUNKS,)),
            dma((nx // 2,)),
            dma((nx,)),
            dma((CHUNKS, nx // 2)),
            dma((CHUNKS, nx)),
            dma((CHUNKS, nx)),
            dma((rounds,)),
            dma((rounds,)),
            dma((ny - 1,)),
            dma((ny - 1,)),
            dma((2, 2)),
            dma((2,)),
        ],
        compiler_params=pltpu.CompilerParams(
            collective_id=0, has_side_effects=True, vmem_limit_bytes=24 * 2**20
        ),
        name="sweeps",
    )(*(v if v is count else pltpu.with_memory_space_constraint(v, pltpu.HBM) for v in operands))
    field = pl.pallas_call(
        add_terms,
        out_shape=jax.ShapeDtypeStruct((2, n, width), F32),
        in_specs=[vmem] * 5 + [smem],
        out_specs=hbm,
        scratch_shapes=[pltpu.VMEM((2, n, width), F32), dma((max(1, width // 256),))],

        compiler_params=pltpu.CompilerParams(vmem_limit_bytes=16 * 2**20),
        name="add_terms",
    )(dexp[0], uexp[0], sources[0], coef, active, count)
    return field[None]


def solution(mesh, ny=4):
    depth, nx = mesh.shape["depth"], mesh.shape["lat"]
    dims = (ny, depth // (2 * ny), nx)
    by_group = P("depth", None, None, "lat")
    return jax.shard_map(
        functools.partial(sweeps, dims),
        mesh=mesh,
        in_specs=(by_group,) * 5
        + (P("depth", None),) * 3
        + (P("depth"),)
        + (P(None, None, "lat"),) * 2,
        out_specs=by_group,
        check_vma=False,
    )
```

```python
import functools

import jax
import jax.numpy as jnp
from jax import lax
from jax.experimental import pallas as pl
from jax.experimental.pallas import tpu as pltpu
from jax.sharding import PartitionSpec as P

F32 = jnp.float32
BF16 = jnp.bfloat16
MESH = pl.DeviceIdType.MESH
CHUNKS = 4


def halves(value):
    high = value.astype(BF16)
    return high, (value - high.astype(F32)).astype(BF16)


def dot(left, right):
    return lax.dot_general(left, right, (((1,), (0,)), ((), ())), preferred_element_type=F32)


def dot_rows(left, right):
    return lax.dot_general(left, right, (((1,), (1,)), ((), ())), preferred_element_type=F32)


def lanes_of(shape):
    return lax.broadcasted_iota(jnp.int32, shape, 1)


def turn(value):
    n = value.shape[1] // 2
    back = pltpu.roll(value, n, 1)
    return jnp.where(lanes_of(value.shape) < n, -back, back)


def product(left, right):
    l_h, l_l = halves(left)
    r_h, r_l = halves(right)
    out = dot(jnp.concatenate([l_h, l_l], axis=1), jnp.concatenate([r_h, r_h], axis=0))
    return out + dot(l_h, r_l)


def apply(later, offset):
    return product(later[0], jnp.concatenate([offset, turn(offset)], axis=0)) + later[1]


def compose(later, earlier):
    both = jnp.concatenate(earlier, axis=1)
    low = jnp.concatenate([turn(earlier[0]), turn(earlier[1])], axis=1)
    out = product(later[0], jnp.concatenate([both, low], axis=0))
    width = earlier[0].shape[1]
    return out[:, :width], out[:, width:] + later[1]


def select(which, first, second):
    return tuple(jnp.where(which, a, b) for a, b in zip(first, second))


def kernel(
    dims,
    src_hbm, dexp_hbm, dproj_hbm, uexp_hbm, uproj_hbm, ddec_hbm, udec_hbm, list_hbm, count_ref, incd_hbm, incu_hbm,
    out_ref,
    src, exps, inc, pown, near, far, wh, wl, fsend, frecv, ssend, srecv, irecv,
    zsend, zrecv, ysend, yrecv, column, qsend, qrecv, ddec_ref, udec_ref, list_ref,
    load_sem, near_sem, far_send_sem, far_recv_sem, fsend_sem, frecv_sem, ssend_sem, srecv_sem, irecv_sem,
    zsend_sem, zrecv_sem, ysend_sem, yrecv_sem, qsend_sem, qrecv_sem,
):
    ny, nz, nx = dims
    rounds = nz.bit_length() - 1
    masks = [(2 << k) - 1 for k in range(rounds)]
    n = src.shape[1]
    size = n // CHUNKS
    width = src.shape[2]
    wide = (n, 2 * n)
    g = lax.axis_index("depth")
    x = lax.axis_index("lat")
    core = lax.rem(g, 2)
    z = lax.rem(lax.div(g, 2), nz)
    y = lax.div(g, 2 * nz)
    mate = g + 1 - 2 * core
    hub = g + 1 - core
    is_hub = core == 1
    sweep = lax.rem(x + 1, 2)
    zz = jnp.where(sweep == 0, z, nz - 1 - z)
    yy = jnp.where(sweep == 0, y, ny - 1 - y)
    begins = jnp.logical_and(yy == 0, zz == 0)
    ends = jnp.logical_and(yy == ny - 1, zz == nz - 1)
    edge = jnp.logical_or(g == 0, g == 2 * ny * nz - 1)
    inner = jnp.logical_not(edge)
    before = jnp.where(edge, g, g - 1 + 2 * core)

    def xor(value, mask):
        out = value
        for bit in range(rounds):
            if mask >> bit & 1:
                out = out + (1 << bit) * (1 - 2 * lax.rem(lax.div(value, 1 << bit), 2))
        return out

    def place(to_y, to_z):
        return (to_y * nz + to_z) * 2 + 1

    z_peers = [place(y, xor(z, mask)) for mask in masks]
    y_peers = [place(jnp.where(sweep == 0, lax.rem(y + o, ny), lax.rem(y + ny - o, ny)), z) for o in range(1, ny)]

    pending = []

    def remote(src_ref, dst_ref, send_sem, recv_sem, to, if_so=None, keep=True):
        copy = pltpu.make_async_remote_copy(
            src_ref=src_ref, dst_ref=dst_ref, send_sem=send_sem, recv_sem=recv_sem,
            device_id=to, device_id_type=MESH,
        )
        if if_so is None:
            copy.start()
        else:
            pl.when(if_so)(copy.start)
        if keep:
            pending.append(copy.wait_send if if_so is None else lambda: pl.when(if_so)(copy.wait_send))
        return copy

    def to_hub(src_ref, dst_ref, send_sem, recv_sem, at, if_so=None):
        itself = jnp.logical_and(is_hub, x == at)
        away = jnp.logical_not(itself)
        if if_so is not None:
            itself, away = jnp.logical_and(itself, if_so), jnp.logical_and(away, if_so)
        copy = remote(src_ref, dst_ref, send_sem, recv_sem, (hub, at), away)
        pl.when(itself)(pltpu.make_async_copy(src_ref, dst_ref, recv_sem).start)
        return copy

    barrier = pltpu.get_barrier_semaphore()

    def greet(group, at):
        pl.semaphore_signal(barrier, inc=1, device_id=(group, at), device_id_type=MESH)

    for o in range(nx):
        greet(mate, lax.rem(x + o, nx))
    pl.when(inner)(lambda: greet(before, x))

    @pl.when(is_hub)
    def _():
        for o in range(1, nx):
            greet(g, lax.rem(x + o, nx))
        for peer in z_peers + y_peers:
            greet(peer, x)

    loads = [
        pltpu.make_async_copy(a, b, load_sem.at[i])
        for i, (a, b) in enumerate(
            [
                (dproj_hbm, pown.at[0]),
                (uproj_hbm, pown.at[1]),
                (dexp_hbm, exps.at[0]),
                (src_hbm, src),
                (uexp_hbm, exps.at[1]),
                (ddec_hbm, ddec_ref),
                (udec_hbm, udec_ref),
                (list_hbm, list_ref),
            ]
        )
    ]
    for copy in loads:
        copy.start()
    inc_copies = [pltpu.make_async_copy(a, inc, load_sem.at[8]) for a in (incd_hbm, incu_hbm)]
    pl.when(jnp.logical_and(edge, core == 0))(inc_copies[0].start)
    pl.when(jnp.logical_and(edge, core == 1))(inc_copies[1].start)

    extra = jnp.where(is_hub, nx - 1 + rounds + ny - 1, 0)
    pl.semaphore_wait(barrier, nx + jnp.where(edge, 0, 1) + extra)

    loads[0].wait()
    loads[1].wait()
    far_copies = []
    for k in range(CHUNKS):
        rows = pl.ds(k * size, size)
        far_copies.append(
            remote(pown.at[core, :, rows], far.at[k], far_send_sem.at[k], far_recv_sem.at[k], (before, x), inner)
        )
        own = pltpu.make_async_copy(pown.at[core, :, rows], far.at[k], far_recv_sem.at[k])
        pl.when(edge)(own.start)
    near_copy = remote(pown.at[1 - core], near, near_sem.at[0], near_sem.at[1], (mate, x))

    for copy in loads[2:]:
        copy.wait()
    square = (n, n)
    row_at = lax.broadcasted_iota(jnp.int32, square, 0)
    lane_at = lanes_of(square)
    valid = jnp.logical_and(list_ref[...] == row_at, lane_at < count_ref[0])
    mask = jnp.sum(jnp.where(valid, 1.0, 0.0), axis=1, keepdims=True)
    for role in range(2):
        first, second = (ddec_ref, udec_ref) if role == 0 else (udec_ref, ddec_ref)
        decay = jnp.where(core == 0, first[...], second[...])
        decay = jnp.sum(jnp.where(row_at == lane_at, decay, 0.0), axis=1, keepdims=True)
        slot = core if role == 0 else 1 - core
        for at in range(2):
            high, low = halves(exps[slot, at] * decay)
            wh[role, pl.ds(at * n, n)] = high
            wl[role, pl.ds(at * n, n)] = low
            high, low = halves(src[at] * mask)
            wh[role, pl.ds((2 + at) * n, n)] = high
            wl[role, pl.ds((2 + at) * n, n)] = low

    @pl.when(edge)
    def _():
        inc_copies[0].wait()
        for at in range(2):
            high, low = halves(inc[at])
            wh[1, pl.ds((2 + at) * n, n)] = high
            wl[1, pl.ds((2 + at) * n, n)] = low

    def meet(right, role):
        rows = right.shape[0] // 2
        p_h, p_l = halves(right)
        both = dot_rows(jnp.concatenate([p_h, p_l], axis=0), wh[role])
        total = both[: 2 * rows] + both[2 * rows :] + dot_rows(p_h, wl[role])
        real, imag = total[:rows], total[rows:]
        return real[:, : 2 * n] + turn(imag[:, : 2 * n]), real[:, 2 * n :] + turn(imag[:, 2 * n :])

    near_copy.wait_recv()
    fsend[0], fsend[1] = meet(near[...].reshape(2 * n, width), 0)
    half = nx // 2
    for j in range(half):
        to_hub(fsend, frecv.at[x], fsend_sem.at[j], frecv_sem.at[x], 1 - core + 2 * j)
    for k in range(CHUNKS):
        far_copies[k].wait_recv()
        ssend[k, 0], ssend[k, 1] = meet(far[k].reshape(2 * size, width), 1)
        for j in range(half):
            sem = ssend_sem.at[k, j]
            to_hub(ssend.at[k], srecv.at[k, x], sem, srecv_sem.at[k, x], core + 2 * j, inner)
            to_hub(ssend.at[k], irecv.at[k, x], sem, irecv_sem.at[k, x], 1 - core + 2 * j, edge)

    def arrived(ref, sem):
        pltpu.make_async_copy(ref, ref, sem).wait()

    def hand_over():
        for at, decay in enumerate((ddec_ref[...], udec_ref[...])):
            arrived(qrecv.at[at], qrecv_sem.at[at])
            columns = qrecv[at]
            turned = jnp.transpose(jnp.concatenate([columns, pltpu.roll(columns, n, 1)], axis=0))[:n]
            out_ref[at] = turned * jnp.concatenate([decay, decay], axis=1)

    lane = lanes_of(wide)

    @pl.when(is_hub)
    def _():
        mine = []
        for at in range(nx):
            arrived(frecv.at[at], frecv_sem.at[at])
        for i in range(2):
            total = frecv[0, i]
            for at in range(1, nx):
                total = total + frecv[at, i]
            mine.append(total)
        mine = tuple(mine)

        @pl.when(begins)
        def _():
            totals = []
            for k in range(CHUNKS):
                for at in range(nx):
                    arrived(irecv.at[k, at], irecv_sem.at[k, at])
                total = irecv[k, 0, 1]
                for at in range(1, nx):
                    total = total + irecv[k, at, 1]
                totals.append(total)
            column[0] = jnp.concatenate(totals, axis=0)
            column[1] = apply(mine, column[0])

        first = select(begins, (jnp.zeros(wide, F32), column[1]), mine)

        @pl.when(jnp.logical_not(ends))
        def _():
            parts = [[], []]
            for k in range(CHUNKS):
                for at in range(nx):
                    arrived(srecv.at[k, at], srecv_sem.at[k, at])
                for i in range(2):
                    total = srecv[k, 0, i]
                    for at in range(1, nx):
                        total = total + srecv[k, at, i]
                    parts[i].append(total)
            theirs = tuple(jnp.concatenate(p, axis=0) for p in parts)
            zsend[0, 0], zsend[0, 1] = compose(theirs, first)

        @pl.when(ends)
        def _():
            zsend[0] = jnp.zeros(zsend.shape[1:], F32)

        row = lax.broadcasted_iota(jnp.int32, wide, 0)
        prefix = (jnp.where(row == lane, 1.0, 0.0), jnp.zeros(wide, F32))
        waits = []

        def pass_on(k):
            copy = remote(
                zsend.at[k], zrecv.at[k], zsend_sem.at[k], zrecv_sem.at[k], (z_peers[k], x), keep=False
            )
            waits.append(copy.wait_send)
            return copy

        y_copies, y_firsts = {}, {}

        def pass_down():
            for o in range(ny - 1, 0, -1):
                to = (y_peers[o - 1], x)
                sems = (ysend_sem.at[o - 1], yrecv_sem.at[o - 1])
                whole = jnp.logical_and(yy > 0, yy + o < ny)
                y_copies[o] = remote(ysend, yrecv.at[o - 1], *sems, to, whole, keep=False)
                y_firsts[o] = remote(ysend.at[1], yrecv.at[o - 1, 1], *sems, to, yy == 0, keep=False)
                waits.append(lambda c=y_copies[o], w=whole: pl.when(w)(c.wait_send))
                waits.append(lambda c=y_firsts[o]: pl.when(yy == 0)(c.wait_send))

        copy = pass_on(0)
        for k in range(rounds):
            total = (zsend[k, 0], zsend[k, 1])
            copy.wait_recv()
            theirs = (zrecv[k, 0], zrecv[k, 1])
            after = lax.rem(lax.div(zz, 1 << k), 2) == 1
            both = compose(select(after, total, theirs), select(after, theirs, total))
            if k + 1 < rounds:
                zsend[k + 1, 0], zsend[k + 1, 1] = both
                copy = pass_on(k + 1)
            else:
                ysend[0], ysend[1] = both
                pass_down()
            prefix = select(after, compose(prefix, theirs) if k else theirs, prefix)

        @pl.when(yy == 0)
        def _():
            qsend[0] = jnp.where(begins, column[0], prefix[1])

        for at in range(1, ny):

            @pl.when(yy == at)
            def _():
                last = prefix
                if at > 2:
                    y_copies[1].wait_recv()
                    last = compose(prefix, (yrecv[0, 0], yrecv[0, 1]))
                y_firsts[at].wait_recv()
                here = yrecv[at - 1, 1]
                for o in range(at - 1, 0 if at <= 2 else 1, -1):
                    y_copies[o].wait_recv()
                    here = apply((yrecv[o - 1, 0], yrecv[o - 1, 1]), here)
                qsend[0] = apply(last, here)

        beside = x - 1 + 2 * sweep
        chip = g - 1
        for i in range(2):
            if i == 1:
                qsend[1] = apply(mine, qsend[0])
            which = sweep if i == 0 else 1 - sweep
            sems = [(qsend_sem.at[i, j], qrecv_sem.at[sweep]) for j in range(2)]
            copy = remote(qsend.at[i], qrecv.at[sweep], *sems[0], (chip + which, beside), keep=False)
            waits.append(copy.wait_send)
            here = which == 0
            copy = remote(qsend.at[i], qrecv.at[sweep], *sems[1], (chip, x), here, keep=False)
            waits.append(lambda c=copy, w=here: pl.when(w)(c.wait_send))
            own = pltpu.make_async_copy(qsend.at[i], qrecv.at[sweep], qrecv_sem.at[sweep])
            pl.when(which == 1)(own.start)
        hand_over()
        for wait in waits:
            wait()

    pl.when(jnp.logical_not(is_hub))(hand_over)
    for wait in pending:
        wait()


def add_terms(dexp, uexp, src, coef, list_ref, count_ref, out_hbm, field, sems):
    _, n, width = src.shape
    square = (n, n)
    valid = jnp.logical_and(
        list_ref[...] == lax.broadcasted_iota(jnp.int32, square, 0), lanes_of(square) < count_ref[0]
    )
    mask = jnp.sum(jnp.where(valid, 1.0, 0.0), axis=1, keepdims=True)
    parts = []
    for sweep in range(2):
        value = coef[sweep]
        left = lanes_of(value.shape) < n
        parts.append(jnp.concatenate([jnp.where(left, value, -value), pltpu.roll(value, n, 1)], axis=0))
    c_h, c_l = halves(jnp.concatenate(parts, axis=1))
    c_all = jnp.concatenate([c_h, c_l], axis=0)
    step = min(512, width)
    copies = []
    for k in range(width // step):
        cols = pl.ds(k * step, step)
        e_h, e_l = halves(
            jnp.concatenate([dexp[:, :, cols].reshape(2 * n, step), uexp[:, :, cols].reshape(2 * n, step)], axis=0)
        )
        both = dot(c_all, e_h)
        terms = both[: 2 * n] + both[2 * n :] + dot(c_h, e_l)
        for i in range(2):
            field[i, :, cols] = src[i, :, cols] * mask + terms[i * n : (i + 1) * n]
        copies.append(pltpu.make_async_copy(field.at[:, :, cols], out_hbm.at[:, :, cols], sems.at[k]))
        copies[-1].start()
    for copy in copies:
        copy.wait()


def sweeps(dims, *args):
    sources, dexp, dproj, uexp, uproj, ddec, udec, active, count, incd, incu = args
    ny, nz, nx = dims
    _, _, n, width = sources.shape
    size = n // CHUNKS
    rounds = nz.bit_length() - 1
    block = (n, 2 * n)
    hbm = pl.BlockSpec(memory_space=pltpu.HBM)
    vmem = pl.BlockSpec(memory_space=pltpu.VMEM)
    smem = pl.BlockSpec(memory_space=pltpu.SMEM)
    dma = pltpu.SemaphoreType.DMA
    operands = (sources[0], dexp[0], dproj[0], uexp[0], uproj[0], ddec, udec, active, count, incd, incu)
    coef = pl.pallas_call(
        functools.partial(kernel, dims),
        out_shape=jax.ShapeDtypeStruct((2, *block), F32),
        in_specs=[hbm] * 8 + [smem] + [hbm] * 2,
        out_specs=vmem,
        scratch_shapes=[
            pltpu.VMEM((2, n, width), F32),
            pltpu.VMEM((2, 2, n, width), F32),
            pltpu.VMEM((2, n, width), F32),
            pltpu.VMEM((2, 2, n, width), F32),
            pltpu.VMEM((2, n, width), F32),
            pltpu.VMEM((CHUNKS, 2, size, width), F32),
            pltpu.VMEM((2, 4 * n, width), BF16),
            pltpu.VMEM((2, 4 * n, width), BF16),
            pltpu.VMEM((2, *block), F32),
            pltpu.VMEM((nx, 2, *block), F32),
            pltpu.VMEM((CHUNKS, 2, size, 2 * n), F32),
            pltpu.VMEM((CHUNKS, nx, 2, size, 2 * n), F32),
            pltpu.VMEM((CHUNKS, nx, 2, size, 2 * n), F32),
            pltpu.VMEM((rounds, 2, *block), F32),
            pltpu.VMEM((rounds, 2, *block), F32),
            pltpu.VMEM((2, *block), F32),
            pltpu.VMEM((ny - 1, 2, *block), F32),
            pltpu.VMEM((2, *block), F32),
            pltpu.VMEM((2, *block), F32),
            pltpu.VMEM((2, *block), F32),
            pltpu.VMEM((1, n), F32),
            pltpu.VMEM((1, n), F32),
            pltpu.VMEM((1, n), jnp.int32),
            dma((9,)),
            dma((2,)),
            dma((CHUNKS,)),
            dma((CHUNKS,)),
            dma((nx // 2,)),
            dma((nx,)),
            dma((CHUNKS, nx // 2)),
            dma((CHUNKS, nx)),
            dma((CHUNKS, nx)),
            dma((rounds,)),
            dma((rounds,)),
            dma((ny - 1,)),
            dma((ny - 1,)),
            dma((2, 2)),
            dma((2,)),
        ],
        compiler_params=pltpu.CompilerParams(
            collective_id=0, has_side_effects=True, vmem_limit_bytes=24 * 2**20
        ),
        name="sweeps",
    )(*(v if v is count else pltpu.with_memory_space_constraint(v, pltpu.HBM) for v in operands))
    field = pl.pallas_call(
        add_terms,
        out_shape=jax.ShapeDtypeStruct((2, n, width), F32),
        in_specs=[vmem] * 5 + [smem],
        out_specs=hbm,
        scratch_shapes=[pltpu.VMEM((2, n, width), F32), dma((max(1, width // 256),))],

        compiler_params=pltpu.CompilerParams(vmem_limit_bytes=16 * 2**20),
        name="add_terms",
    )(dexp[0], uexp[0], sources[0], coef, active, count)
    return field[None]


def solution(mesh, ny=4):
    depth, nx = mesh.shape["depth"], mesh.shape["lat"]
    dims = (ny, depth // (2 * ny), nx)
    by_group = P("depth", None, None, "lat")
    return jax.shard_map(
        functools.partial(sweeps, dims),
        mesh=mesh,
        in_specs=(by_group,) * 5
        + (P("depth", None),) * 3
        + (P("depth"),)
        + (P(None, None, "lat"),) * 2,
        out_specs=by_group,
        check_vma=False,
    )
```
